32 devices in a mesh: af: 16 (over z, y, x), sa: 2 (over core).
Axes of the slice: x: 2, y: 2, z: 4, core: 2. Of those that a mesh axis runs over, the one named last changes fastest.
Arguments:
- series: float32 [8, 262144], P('sa', 'af'), parts along dimension 0, may hold values from -48 to 48
- tapers: float32 [10, 262144], P(None, 'af'), may hold values from -16 to 16
- concentration: float32 [10], replicated, may hold values from 0.2 to 0.95
- qi_weights: float32 [4, 10, 10], replicated, may hold values from -0.625 to 0.625
Outputs:
- spectrum: float32 [8, 16, 16384], P('sa', 'af'), parts along dimension 0
- qi_terms: float32 [8, 4, 16, 16384], P('sa', None, 'af'), parts along dimension 0
The draws below stay inside these ranges and needn't reach their ends.
There are 2 independent parts, one for each index of `sa`. The reference program is written for one: setup_inputs(seed, part) draws one part's arguments, and reference() takes and returns one part's arrays. A program takes and returns all parts, laid end to end along the dimension named above; an argument that names none is the same for every part. Nothing has to cross between parts.
All inputs are finite; a program needn't handle non-finite values.
Results may differ from the reference program's by a relative error of at most 0.0001.
Values sent between devices are 32-bit elements; how exact they have to be, the bound alone decides.
A program may use at most 128 MiB of HBM per device.

```python
import math
import jax
import jax.numpy as jnp
from jax import lax

K = 10
L = 4
ITERS = 3
SERIES = 4
TIME_DEV = 16384
SAMPLES = 262144
N_AF = 16


def draw_series(key, part):
    noise_key = jax.random.fold_in(key, 17)
    cycle_key = jax.random.fold_in(key, 29)
    time_frac = jnp.arange(SAMPLES, dtype=jnp.float32) / SAMPLES
    period = SAMPLES // TIME_DEV
    noise_part = jnp.clip(jax.random.normal(noise_key, (SERIES, SAMPLES), jnp.float32), -6.0, 6.0)
    memory_coef = 0.9
    envelope = jnp.exp(math.log(3.0) * time_frac)
    cycle_part = jnp.clip(jax.random.normal(cycle_key, (SERIES, TIME_DEV), jnp.float32), -4.0, 4.0)
    strength = 3.0
    shifted = jnp.roll(noise_part, 1, axis=1)
    repeated = jnp.tile(cycle_part, (1, period))
    return ((noise_part + memory_coef * shifted) * envelope[None, :] + strength * repeated).astype(jnp.float32)


def draw_tapers(key, part):
    coef_key = jax.random.fold_in(key, 41)
    rough_key = jax.random.fold_in(key, 43)
    harmonic_count = K + 2
    positions = (jnp.arange(SAMPLES, dtype=jnp.float32) + 1.0) / (SAMPLES + 1)
    harmonics = jnp.arange(1, harmonic_count + 1, dtype=jnp.float32)
    sine_basis = jnp.sin(math.pi * harmonics[:, None] * positions[None, :])
    coeffs = jnp.clip(jax.random.normal(coef_key, (K, harmonic_count), jnp.float32), -3.0, 3.0) * math.sqrt(2.0 / harmonic_count)
    rough_part = jnp.clip(jax.random.normal(rough_key, (K, SAMPLES), jnp.float32), -4.0, 4.0) * 0.15
    smooth = jnp.dot(coeffs, sine_basis, precision=lax.Precision.HIGHEST)
    return (smooth + rough_part).astype(jnp.float32)


def noise(own_key, extent, width, reach, kind=jnp.bfloat16):
    return jnp.clip(width * jax.random.normal(own_key, extent, jnp.float32), -reach, reach).astype(kind)


def setup_inputs(seed: int = 0, part: int = 0) -> dict:
    keys = jax.random.split(jax.random.key(seed), 5)
    part_keys = jax.random.split(jax.random.fold_in(keys[4], part), 5)
    return {
        "series": draw_series(jax.random.fold_in(jax.random.fold_in(keys[4], part), 71), part),
        "tapers": draw_tapers(jax.random.fold_in(keys[4], 71), part),
        "concentration": jnp.clip(jax.random.uniform(keys[2], (K,), jnp.float32, 0.2, 0.95), 0.2, 0.95),
        "qi_weights": noise(keys[3], (L, K, K), (K * K) ** -0.5, 0.625, jnp.float32),
    }


def reference(series, tapers, concentration, qi_weights):
    highest = lax.Precision.HIGHEST
    retained = concentration[:, None]
    unit_scale = 1.0 / math.sqrt(SAMPLES)
    spectra = []
    term_list = []
    for series_index in range(SERIES):
        scaled = series[series_index] * unit_scale
        coeffs = jnp.fft.fft(tapers * scaled[None, :], axis=1)
        coeffs = coeffs.reshape(K, TIME_DEV, N_AF).transpose(0, 2, 1).reshape(K, SAMPLES)
        real_part = jnp.real(coeffs)
        imag_part = jnp.imag(coeffs)
        powers = real_part * real_part + imag_part * imag_part
        per_term = []
        for term_index in range(L):
            mixed_re = jnp.dot(qi_weights[term_index], real_part, precision=highest)
            mixed_im = jnp.dot(qi_weights[term_index], imag_part, precision=highest)
            per_term.append(lax.optimization_barrier(jnp.sum(real_part * mixed_re + imag_part * mixed_im, axis=0)))
        estimate = 0.5 * (powers[0] + powers[1])
        for sweep_index in range(ITERS):
            variance = jnp.mean(estimate)
            weight = retained / (retained * estimate[None, :] + (1.0 - retained) * variance) ** 2
            estimate = lax.optimization_barrier(jnp.sum(weight * powers, axis=0)) / lax.optimization_barrier(jnp.sum(weight, axis=0))
        spectra.append(estimate.reshape(N_AF, TIME_DEV))
        term_list.append(jnp.stack(per_term).reshape(L, N_AF, TIME_DEV))
    return (jnp.stack(spectra), jnp.stack(term_list))
```

```python
import functools
import math

import jax
import jax.numpy as jnp
import numpy as np
from jax import lax
from jax.experimental import pallas as pl
from jax.experimental.pallas import tpu as pltpu
from jax.sharding import PartitionSpec as P

ITERS = 3
LANES = 128
CHUNK = 16
MESH = pl.DeviceIdType.MESH


def add(a, b):
    if a is None:
        return b
    return a if b is None else a + b


def sub(a, b):
    if b is None:
        return a
    return -b if a is None else a - b


def butterfly(values):
    n = len(values)
    if n == 1:
        return values
    even, odd = butterfly(values[0::2]), butterfly(values[1::2])
    low, high = [], []
    for k in range(n // 2):
        (er, ei), (tr, ti) = even[k], odd[k]
        if 4 * k == n:
            tr, ti = ti, (None if tr is None else -tr)
        elif k:
            c, s = math.cos(2 * math.pi * k / n), math.sin(2 * math.pi * k / n)
            if ti is None:
                tr, ti = tr * c, tr * (-s)
            else:
                tr, ti = tr * c + ti * s, ti * c - tr * s
        low.append((add(er, tr), add(ei, ti)))
        high.append((sub(er, tr), sub(ei, ti)))
    return low + high


def split(x):
    high = x.astype(jnp.bfloat16)
    return high, (x - high.astype(jnp.float32)).astype(jnp.bfloat16)


def dot3(a, b):
    dot = functools.partial(jnp.dot, preferred_element_type=jnp.float32)
    return dot(a[0], b[0]) + (dot(a[0], b[1]) + dot(a[1], b[0]))


def refine(estimate, powers, keep, variance):
    top = bottom = None
    for k, power in enumerate(powers):
        base = keep[k] * estimate + (1.0 - keep[k]) * variance
        weight = keep[k] / (base * base)
        top = add(top, weight * power)
        bottom = add(bottom, weight)
    return top / bottom


def turn(index, period):
    if period & (period - 1):
        index = lax.rem(index, jnp.full_like(index, period))
    else:
        index = index & (period - 1)
    angle = index.astype(jnp.float32) * (2.0 * math.pi / period)
    return jnp.cos(angle), jnp.sin(angle)


def flip(x):
    rows, lanes = x.shape
    lane = lanes - 1 - lax.broadcasted_iota(jnp.int32, (8, lanes), 1)
    line = 7 - lax.broadcasted_iota(jnp.int32, (8, lanes), 0)
    parts = []
    for i in reversed(range(rows // 8)):
        part = jnp.take_along_axis(x[8 * i : 8 * i + 8], lane, axis=1)
        parts.append(jnp.take_along_axis(part, line, axis=0))
    return jnp.concatenate(parts, axis=0)


def remote(src, dst, send, recv, where):
    return pltpu.make_async_remote_copy(
        src_ref=src, dst_ref=dst, send_sem=send, recv_sem=recv, device_id=where, device_id_type=MESH
    )


def fused_kernel(
    n, cores, series_ref, tapers_ref, keep_ref, mix_ref, spec_ref, qi_ref,
    ser, tap, zbuf, recv, en_out, en_in, sum_out, sum_in, left, right, inner, weigh,
    spec, power, est, qi, spec_out, qi_out, pairs, folded,
    ser_ss, ser_rs, tap_ss, tap_rs, core_ss, core_rs, en_ss, en_rs, z_ss, z_rs,
    sum_ss, sum_rs, qo_ss, qo_rs, so_ss, so_rs,
):
    half = n // 2
    count, sub_rows = series_ref.shape[0], series_ref.shape[2]
    mine = count // 2
    tapers, terms = tap.shape[1], mix_ref.shape[0]
    group = tapers // cores
    rows = half * sub_rows
    tall = spec.shape[2]
    extra = tall - rows
    local_len = rows * LANES
    length_all = local_len * n
    f32 = jnp.float32
    me, core = lax.axis_index("af"), lax.axis_index("sa")
    g, h = me // half, lax.rem(me, half)
    peers = [(dg, dh) for dg in (1, 0) for dh in range(half) if dg or dh]
    single = h == 0

    def ahead(dg, dh):
        return lax.rem(g + dg, 2), lax.rem(h + dh, half)

    def behind(dg, dh):
        return lax.rem(g + dg, 2), lax.rem(h + half - dh, half)

    def flat(at):
        return at[0] * half + at[1]

    def friend(dh):
        return {"af": g * half + lax.rem(h + dh, half)}

    partner = {"af": (1 - g) * half + lax.rem(half - h, half)}
    other_core = lax.rem(core + 1, cores)

    barrier = pltpu.get_barrier_semaphore()
    for dg, dh in peers:
        pl.semaphore_signal(barrier, inc=1, device_id={"af": flat(ahead(dg, dh))}, device_id_type=MESH)
    pl.semaphore_signal(barrier, inc=1, device_id={"sa": other_core}, device_id_type=MESH)
    pl.semaphore_wait(barrier, n)

    def ser_copy(dg, dh):
        to = ahead(dg, dh)
        return remote(
            series_ref.at[pl.ds(to[0] * mine, mine), to[1]], ser.at[me],
            ser_ss.at[dg, dh], ser_rs.at[dg, dh], {"af": flat(to)},
        )

    def tap_copy(dg, dh):
        to = ahead(dg, dh)
        own = pl.ds(core * group, group)
        return remote(
            tapers_ref.at[own, to[1]], tap.at[me, own],
            tap_ss.at[dg, dh], tap_rs.at[dg, dh], {"af": flat(to)},
        )

    def core_copy(dg, dh):
        at = tap.at[flat(behind(dg, dh)), pl.ds(core * group, group)]
        return remote(at, at, core_ss.at[dg, dh], core_rs.at[dg, dh], {"sa": other_core})

    for dg, dh in peers:
        tap_copy(dg, dh).start()
        ser_copy(dg, dh).start()

    for s in range(mine):
        ser[me, s] = series_ref[g * mine + s, h]
    for k in range(tapers):
        tap[me, k] = tapers_ref[k, h]
    for t in range(terms):
        p = 0
        for j in range(tapers):
            for k in range(j, tapers):
                value = mix_ref[t, j, k]
                pairs[t, p] = value if j == k else value + mix_ref[t, k, j]
                p += 1

    def frequency(shape):
        at = lax.broadcasted_iota(jnp.int32, shape, 0)
        upper = (at >= rows // 2) & (at < rows)
        class_of = jnp.where(single, jnp.where(upper, half, 0), me)
        line = jnp.where(at < rows, at, rows // 2)
        class_of = jnp.where(at < rows, class_of, 0)
        return n * line + class_of, at, upper

    freq, at, upper = frequency((tall, rows))
    c, s = turn(lax.broadcasted_iota(jnp.int32, (tall, rows), 1) * freq, rows * n)
    first = jnp.where(upper, 1, 0) == g
    inside = at < rows
    once = at == rows
    zero = jnp.zeros_like(c)
    take0 = jnp.where(single, jnp.where(inside | once, jnp.where(first, 1.0, 0.0), 0.0), jnp.where(inside, 1.0, 0.0))
    take1 = jnp.where(single, jnp.where(inside | once, jnp.where(first, 0.0, 1.0), 0.0), 0.0)
    plain = jnp.where(single, 0.0, jnp.where(inside, 1.0, 0.0))
    real0, real1 = c * take0, c * take1 + s * plain
    imag0, imag1 = -(s * take0), c * plain - s * take1
    full = jnp.concatenate(
        [
            jnp.concatenate([real0[:rows], real1[:rows]], axis=1),
            jnp.concatenate([imag0[:rows], imag1[:rows]], axis=1),
            jnp.concatenate([real0[rows:], real1[rows:]], axis=1),
        ],
        axis=0,
    )
    left[0], left[1] = split(full)

    freq, at, upper = frequency((tall, LANES))
    c, s = turn(lax.broadcasted_iota(jnp.int32, (tall, LANES), 1) * freq, length_all)
    scale = 1.0 / math.sqrt(length_all)
    inner[0], inner[1] = c * scale, s * scale
    weigh[...] = jnp.where(
        single,
        jnp.where(at < rows, jnp.where(at == 0, 1.0, 2.0), jnp.where(at == rows, 1.0, 0.0)),
        jnp.where(at < rows, 2.0, 0.0),
    )
    grid = (LANES, LANES)
    c, s = turn(lax.broadcasted_iota(jnp.int32, grid, 0) * lax.broadcasted_iota(jnp.int32, grid, 1), LANES)
    right[0], right[1] = split(
        jnp.concatenate([jnp.concatenate([c, -s], axis=1), jnp.concatenate([s, c], axis=1)], axis=0)
    )
    en_out[...] = jnp.zeros_like(en_out)
    sum_out[...] = jnp.zeros_like(sum_out)

    for dg, dh in peers:
        tap_copy(dg, dh).wait_recv()
        core_copy(dg, dh).start()
    for dg, dh in peers:
        ser_copy(dg, dh).wait_recv()
    for dg, dh in peers:
        core_copy(dg, dh).wait_recv()

    def energy(p, total):
        one, two = tap[p, 0], tap[p, 1]
        new = []
        for s in range(mine):
            a, b = ser[p, s] * one, ser[p, s] * two
            new.append(total[s] + (a * a + b * b))
        return tuple(new)

    total = lax.fori_loop(0, n, energy, tuple(jnp.zeros((sub_rows, LANES), f32) for _ in range(mine)))
    for s in range(mine):
        en_out[s : s + 1] = jnp.sum(total[s], axis=0, keepdims=True)

    def en_copy(dh):
        return remote(en_out, en_in.at[dh], en_ss.at[dh], en_rs.at[dh], friend(dh))

    for dh in range(1, half):
        en_copy(dh).start()

    def z_copy(s, dh):
        to = lax.rem(h + dh, half)
        return remote(
            zbuf.at[to, s], recv.at[s, :, :, h], z_ss.at[s, dh], z_rs.at[s, dh], friend(dh)
        )

    sign = (1 - 2 * g).astype(f32)
    tile = min(8, sub_rows)
    for s in range(mine):
        for i in range(sub_rows // tile):
            part = pl.ds(i * tile, tile)

            def front(k, carry, s=s, part=part):
                got = []
                for p in range(n):
                    value = ser[p, s, part] * tap[p, k, part]
                    got.append((value * sign if p % 2 else value, None))
                out = butterfly(got)
                for u in range(half):
                    re, im = out[u]
                    zbuf[u, s, k, 0, part] = re
                    zbuf[u, s, k, 1, part] = out[half][0] if u == 0 else im
                return carry

            lax.fori_loop(0, tapers, front, 0)
        for dh in range(1, half):
            z_copy(s, dh).start()
        for k in range(tapers):
            for part in range(2):
                recv[s, k, part, h] = zbuf[h, s, k, part]

    for dh in range(1, half):
        en_copy(dh).wait_recv()
    total = en_out[...]
    for dh in range(1, half):
        total += en_in[dh]
    variance0 = [jnp.sum(total[s : s + 1]) * (0.5 / length_all) for s in range(mine)]
    keep = [keep_ref[k] for k in range(tapers)]

    def sum_copy(s, it, dh):
        return remote(
            sum_out.at[s, it], sum_in.at[s, it, dh], sum_ss.at[s, it, dh], sum_rs.at[s, it, dh], friend(dh)
        )

    def share(s, it, total):
        sum_out[s, it, 0:1] = jnp.sum(total, axis=0, keepdims=True)
        for dh in range(1, half):
            sum_copy(s, it, dh).start()

    def collect(s, it):
        total = sum_out[s, it]
        for dh in range(1, half):
            sum_copy(s, it, dh).wait_recv()
            total += sum_in[s, it, dh]
        return jnp.sum(total) / length_all

    def transform(s):
        def body(kk, carry):
            k = 2 * kk
            x = jnp.concatenate(
                [recv[s, k].reshape(2 * rows, LANES), recv[s, k + 1].reshape(2 * rows, LANES)], axis=1
            )
            mid = dot3((left[0], left[1]), split(x))
            c, d = inner[0], inner[1]
            turned = []
            for i in range(2):
                lanes = slice(i * LANES, (i + 1) * LANES)
                mr = jnp.concatenate([mid[:rows, lanes], mid[2 * rows :, lanes]], axis=0)
                mi = jnp.concatenate([mid[rows : 2 * rows, lanes], jnp.zeros((extra, LANES), f32)], axis=0)
                turned.append(jnp.concatenate([mr * c + mi * d, mi * c - mr * d], axis=1))
            done = dot3(split(jnp.concatenate(turned, axis=0)), (right[0], right[1]))
            for i in range(2):
                block = done[i * tall : (i + 1) * tall]
                spec[0, k + i] = block[:, :LANES]
                spec[1, k + i] = block[:, LANES:]
            return carry

        lax.fori_loop(0, tapers // 2, body, 0)

    def combine(s, variance):
        def body(i, total):
            at = pl.ds(pl.multiple_of(i * CHUNK, CHUNK), CHUNK)
            re = [spec[0, k, at] for k in range(tapers)]
            im = [spec[1, k, at] for k in range(tapers)]
            sums = [None] * terms
            powers = []
            pair = 0
            for j in range(tapers):
                for k in range(j, tapers):
                    both = re[j] * re[k] + im[j] * im[k]
                    if j == k:
                        powers.append(both)
                        power[s, k, at] = both
                    for t in range(terms):
                        sums[t] = add(sums[t], pairs[t, pair] * both)
                    pair += 1
            for t in range(terms):
                qi[s, t, at] = sums[t]
            new = refine(0.5 * (powers[0] + powers[1]), powers, keep, variance)
            est[s, at] = new
            return total + new * weigh[at]

        return lax.fori_loop(0, tall // CHUNK, body, jnp.zeros((CHUNK, LANES), f32))

    def sweep(s, variance):
        def body(i, total):
            at = pl.ds(pl.multiple_of(i * CHUNK, CHUNK), CHUNK)
            new = refine(est[s, at], [power[s, k, at] for k in range(tapers)], keep, variance)
            est[s, at] = new
            return total + new * weigh[at]

        return lax.fori_loop(0, tall // CHUNK, body, jnp.zeros((CHUNK, LANES), f32))

    def assemble(src):
        mirrored = flip(src[0:rows])

        @pl.when(jnp.logical_not(single))
        def _():
            folded[0] = src[0:rows]
            folded[1] = mirrored

        @pl.when(single)
        def _():
            folded[g, 0 : rows // 2] = src[0 : rows // 2]
            folded[g, rows // 2 : rows // 2 + 1] = src[rows : rows + 1]
            folded[g, rows // 2 + 1 : rows] = mirrored[rows // 2 : rows - 1]
            folded[1 - g, 0 : rows // 2] = mirrored[: rows // 2]
            folded[1 - g, rows // 2 : rows] = src[rows // 2 : rows]

        return folded[0].T, folded[1].T

    def qi_copy(s):
        return remote(qi_out.at[s], qi_ref.at[g * mine + s], qo_ss.at[s], qo_rs.at[s], partner)

    def spec_copy(s):
        return remote(spec_out.at[s], spec_ref.at[g * mine + s], so_ss.at[s], so_rs.at[s], partner)

    def outputs_qi(s):
        for t in range(terms):
            own, sent = assemble(qi.at[s, t])
            qi_ref[g * mine + s, t] = own
            qi_out[s, t] = sent
        qi_copy(s).start()

    def outputs_spec(s):
        own, sent = assemble(est.at[s])
        spec_ref[g * mine + s] = own
        spec_out[s] = sent
        spec_copy(s).start()

    for s in range(mine):
        for dh in range(1, half):
            z_copy(s, dh).wait_recv()
        transform(s)
        share(s, 0, combine(s, variance0[s]))
        outputs_qi(s)
        for it in range(1, ITERS):
            total = sweep(s, collect(s, it - 1))
            if it < ITERS - 1:
                share(s, it, total)
        outputs_spec(s)

    for s in range(mine):
        qi_copy(s).wait_recv()
        spec_copy(s).wait_recv()
        qi_copy(s).wait_send()
        spec_copy(s).wait_send()
        for dh in range(1, half):
            z_copy(s, dh).wait_send()
            for it in range(ITERS - 1):
                sum_copy(s, it, dh).wait_send()
    for dh in range(1, half):
        en_copy(dh).wait_send()
    for dg, dh in peers:
        tap_copy(dg, dh).wait_send()
        ser_copy(dg, dh).wait_send()
        core_copy(dg, dh).wait_send()


def local(cores, series, tapers, concentration, qi_weights):
    n = lax.axis_size("af")
    count, local_len = series.shape
    taper_count = tapers.shape[0]
    terms = qi_weights.shape[0]
    half, mine = n // 2, count // 2
    sub_rows = local_len // (half * LANES)
    rows = local_len // LANES
    tall = rows + CHUNK
    f32 = jnp.float32
    bf16 = jnp.bfloat16
    vmem = pl.BlockSpec(memory_space=pltpu.VMEM)
    smem = pl.BlockSpec(memory_space=pltpu.SMEM)
    dma = pltpu.SemaphoreType.DMA
    spectrum, qi_terms = pl.pallas_call(
        functools.partial(fused_kernel, n, cores),
        out_shape=(
            jax.ShapeDtypeStruct((count, LANES, rows), f32),
            jax.ShapeDtypeStruct((count, terms, LANES, rows), f32),
        ),
        in_specs=[vmem, vmem, smem, smem],
        out_specs=(vmem, vmem),
        scratch_shapes=[
            pltpu.VMEM((n, mine, sub_rows, LANES), f32),
            pltpu.VMEM((n, taper_count, sub_rows, LANES), f32),
            pltpu.VMEM((half, mine, taper_count, 2, sub_rows, LANES), f32),
            pltpu.VMEM((mine, taper_count, 2, half, sub_rows, LANES), f32),
            pltpu.VMEM((8, LANES), f32),
            pltpu.VMEM((half, 8, LANES), f32),
            pltpu.VMEM((mine, ITERS - 1, 8, LANES), f32),
            pltpu.VMEM((mine, ITERS - 1, half, 8, LANES), f32),
            pltpu.VMEM((2, rows + tall, 2 * rows), bf16),
            pltpu.VMEM((2, 2 * LANES, 2 * LANES), bf16),
            pltpu.VMEM((2, tall, LANES), f32),
            pltpu.VMEM((tall, LANES), f32),
            pltpu.VMEM((2, taper_count, tall, LANES), f32),
            pltpu.VMEM((mine, taper_count, tall, LANES), f32),
            pltpu.VMEM((mine, tall, LANES), f32),
            pltpu.VMEM((mine, terms, tall, LANES), f32),
            pltpu.VMEM((mine, LANES, rows), f32),
            pltpu.VMEM((mine, terms, LANES, rows), f32),
            pltpu.SMEM((terms, taper_count * (taper_count + 1) // 2), f32),
            pltpu.VMEM((2, rows, LANES), f32),
            dma((2, half)), dma((2, half)),
            dma((2, half)), dma((2, half)),
            dma((2, half)), dma((2, half)),
            dma((half,)), dma((half,)),
            dma((mine, half)), dma((mine, half)),
            dma((mine, ITERS - 1, half)), dma((mine, ITERS - 1, half)),
            dma((mine,)), dma((mine,)),
            dma((mine,)), dma((mine,)),
        ],
        compiler_params=pltpu.CompilerParams(collective_id=0, has_side_effects=True),
    )(
        series.reshape(count, half, sub_rows, LANES),
        tapers.reshape(taper_count, half, sub_rows, LANES),
        concentration,
        qi_weights,
    )
    return (
        spectrum.reshape(count, 1, local_len),
        qi_terms.reshape(count, terms, 1, local_len),
    )


def solution(mesh):
    placed = (P("sa", "af"), P(None, "af"), P(), P())
    return jax.shard_map(
        functools.partial(local, mesh.shape["sa"]),
        mesh=mesh,
        in_specs=placed,
        out_specs=(P("sa", "af", None), P("sa", None, "af", None)),
        check_vma=False,
    )
```

```python
import functools
import math

import jax
import jax.numpy as jnp
import numpy as np
from jax import lax
from jax.experimental import pallas as pl
from jax.experimental.pallas import tpu as pltpu
from jax.sharding import PartitionSpec as P

ITERS = 3
LANES = 128
CHUNK = 16
MESH = pl.DeviceIdType.MESH


def add(a, b):
    if a is None:
        return b
    return a if b is None else a + b


def sub(a, b):
    if b is None:
        return a
    return -b if a is None else a - b


def butterfly(values):
    n = len(values)
    if n == 1:
        return values
    even, odd = butterfly(values[0::2]), butterfly(values[1::2])
    low, high = [], []
    for k in range(n // 2):
        (er, ei), (tr, ti) = even[k], odd[k]
        if 4 * k == n:
            tr, ti = ti, (None if tr is None else -tr)
        elif k:
            c, s = math.cos(2 * math.pi * k / n), math.sin(2 * math.pi * k / n)
            if ti is None:
                tr, ti = tr * c, tr * (-s)
            else:
                tr, ti = tr * c + ti * s, ti * c - tr * s
        low.append((add(er, tr), add(ei, ti)))
        high.append((sub(er, tr), sub(ei, ti)))
    return low + high


def split(x):
    high = x.astype(jnp.bfloat16)
    return high, (x - high.astype(jnp.float32)).astype(jnp.bfloat16)


def dot3(a, b):
    dot = functools.partial(jnp.dot, preferred_element_type=jnp.float32)
    return dot(a[0], b[0]) + (dot(a[0], b[1]) + dot(a[1], b[0]))


def refine(estimate, powers, keep, variance):
    top = bottom = None
    for k, power in enumerate(powers):
        base = keep[k] * estimate + (1.0 - keep[k]) * variance
        weight = keep[k] / (base * base)
        top = add(top, weight * power)
        bottom = add(bottom, weight)
    return top / bottom


def turn(index, period):
    if period & (period - 1):
        index = lax.rem(index, jnp.full_like(index, period))
    else:
        index = index & (period - 1)
    angle = index.astype(jnp.float32) * (2.0 * math.pi / period)
    return jnp.cos(angle), jnp.sin(angle)


def flip(x):
    rows, lanes = x.shape
    lane = lanes - 1 - lax.broadcasted_iota(jnp.int32, (8, lanes), 1)
    line = 7 - lax.broadcasted_iota(jnp.int32, (8, lanes), 0)
    parts = []
    for i in reversed(range(rows // 8)):
        part = jnp.take_along_axis(x[8 * i : 8 * i + 8], lane, axis=1)
        parts.append(jnp.take_along_axis(part, line, axis=0))
    return jnp.concatenate(parts, axis=0)


def remote(src, dst, send, recv, where):
    return pltpu.make_async_remote_copy(
        src_ref=src, dst_ref=dst, send_sem=send, recv_sem=recv, device_id=where, device_id_type=MESH
    )


def fused_kernel(
    n, cores, lead, series_ref, tapers_ref, keep_ref, mix_ref, spec_ref, qi_ref,
    stage, ser_src, tap_src, ser, tap, zbuf, recv, en_out, en_in, sum_out, sum_in, left, right, inner, weigh,
    spec, power, est, qi, spec_out, qi_out, pairs, folded,
    ser_ss, ser_rs, tap_ss, tap_rs, core_ss, core_rs, en_ss, en_rs, z_ss, z_rs,
    sum_ss, sum_rs, qo_ss, qo_rs, so_ss, so_rs,
):
    half = n // 2
    count, sub_rows = ser_src.shape[0], ser_src.shape[2]
    mine = count // 2
    tapers, terms = tap.shape[1], mix_ref.shape[1]
    group = tapers // cores
    sizes = (lead, group - lead)
    starts = (0, lead)
    places = (0, cores * lead)
    order = [c * group + starts[b] + i for b in range(2) for c in range(cores) for i in range(sizes[b])]
    rows = half * sub_rows
    tall = spec.shape[2]
    extra = tall - rows
    local_len = rows * LANES
    length_all = local_len * n
    tile = min(8, sub_rows)
    f32 = jnp.float32
    me, core = lax.axis_index("af"), lax.axis_index("sa")
    g, h = me // half, lax.rem(me, half)
    peers = [(dg, dh) for dg in (1, 0) for dh in range(half) if dg or dh]
    single = h == 0

    def ahead(dg, dh):
        return lax.rem(g + dg, 2), lax.rem(h + dh, half)

    def behind(dg, dh):
        return lax.rem(g + dg, 2), lax.rem(h + half - dh, half)

    def flat(at):
        return at[0] * half + at[1]

    def friend(dh):
        return {"af": g * half + lax.rem(h + dh, half)}

    partner = {"af": (1 - g) * half + lax.rem(half - h, half)}
    other_core = lax.rem(core + 1, cores)

    barrier = pltpu.get_barrier_semaphore()
    for dg, dh in peers:
        pl.semaphore_signal(barrier, inc=1, device_id={"af": flat(ahead(dg, dh))}, device_id_type=MESH)
    pl.semaphore_signal(barrier, inc=1, device_id={"sa": other_core}, device_id_type=MESH)

    for j in range(rows):
        lanes = slice(j * LANES, (j + 1) * LANES)
        stage[0, 8 * j : 8 * j + 8] = tapers_ref[0:8, lanes]
        stage[1, 8 * j : 8 * j + tapers - 8] = tapers_ref[8:tapers, lanes]
        stage[1, 8 * j + tapers - 8 : 8 * j + tapers - 8 + count] = series_ref[:, lanes]
    for row in range(tapers + count):
        for j in range(rows // tile):
            part = stage[row // 8, pl.ds(8 * j * tile + row % 8, tile, stride=8)]
            at = (j * tile // sub_rows, slice(j * tile % sub_rows, j * tile % sub_rows + tile))
            if row < tapers:
                tap_src[row, at[0], at[1]] = part
            else:
                ser_src[row - tapers, at[0], at[1]] = part
    pl.semaphore_wait(barrier, n)

    def ser_copy(dg, dh):
        to = ahead(dg, dh)
        return remote(
            ser_src.at[pl.ds(to[0] * mine, mine), to[1]], ser.at[me],
            ser_ss.at[dg, dh], ser_rs.at[dg, dh], {"af": flat(to)},
        )

    def tap_copy(b, dg, dh):
        to = ahead(dg, dh)
        return remote(
            tap_src.at[pl.ds(core * group + starts[b], sizes[b]), to[1]],
            tap.at[me, pl.ds(places[b] + core * sizes[b], sizes[b])],
            tap_ss.at[b, dg, dh], tap_rs.at[b, dg, dh], {"af": flat(to)},
        )

    def core_copy(b, dg, dh):
        at = tap.at[flat(behind(dg, dh)), pl.ds(places[b] + core * sizes[b], sizes[b])]
        return remote(at, at, core_ss.at[b, dg, dh], core_rs.at[b, dg, dh], {"sa": other_core})

    for dg, dh in peers:
        ser_copy(dg, dh).start()
        tap_copy(0, dg, dh).start()
    for dg, dh in peers:
        tap_copy(1, dg, dh).start()

    for s in range(mine):
        ser[me, s] = ser_src[g * mine + s, h]
    for i, k in enumerate(order):
        tap[me, i] = tap_src[k, h]
    for t in range(terms):
        p = 0
        for j in range(tapers):
            for k in range(j, tapers):
                value = mix_ref[order[j], t, order[k]]
                pairs[t, p] = value if j == k else value + mix_ref[order[k], t, order[j]]
                p += 1

    def frequency(shape):
        at = lax.broadcasted_iota(jnp.int32, shape, 0)
        upper = (at >= rows // 2) & (at < rows)
        class_of = jnp.where(single, jnp.where(upper, half, 0), me)
        line = jnp.where(at < rows, at, rows // 2)
        class_of = jnp.where(at < rows, class_of, 0)
        return n * line + class_of, at, upper

    freq, at, upper = frequency((tall, rows))
    c, s = turn(lax.broadcasted_iota(jnp.int32, (tall, rows), 1) * freq, rows * n)
    first = jnp.where(upper, 1, 0) == g
    inside = at < rows
    once = at == rows
    take0 = jnp.where(single, jnp.where(inside | once, jnp.where(first, 1.0, 0.0), 0.0), jnp.where(inside, 1.0, 0.0))
    take1 = jnp.where(single, jnp.where(inside | once, jnp.where(first, 0.0, 1.0), 0.0), 0.0)
    plain = jnp.where(single, 0.0, jnp.where(inside, 1.0, 0.0))
    real0, real1 = c * take0, c * take1 + s * plain
    imag0, imag1 = -(s * take0), c * plain - s * take1
    full = jnp.concatenate(
        [
            jnp.concatenate([real0[:rows], real1[:rows]], axis=1),
            jnp.concatenate([imag0[:rows], imag1[:rows]], axis=1),
            jnp.concatenate([real0[rows:], real1[rows:]], axis=1),
        ],
        axis=0,
    )
    left[0], left[1] = split(full)

    freq, at, upper = frequency((tall, LANES))
    c, s = turn(lax.broadcasted_iota(jnp.int32, (tall, LANES), 1) * freq, length_all)
    scale = 1.0 / math.sqrt(length_all)
    inner[0], inner[1] = c * scale, s * scale
    weigh[...] = jnp.where(
        single,
        jnp.where(at < rows, jnp.where(at == 0, 1.0, 2.0), jnp.where(at == rows, 1.0, 0.0)),
        jnp.where(at < rows, 2.0, 0.0),
    )
    grid = (LANES, LANES)
    c, s = turn(lax.broadcasted_iota(jnp.int32, grid, 0) * lax.broadcasted_iota(jnp.int32, grid, 1), LANES)
    right[0], right[1] = split(
        jnp.concatenate([jnp.concatenate([c, -s], axis=1), jnp.concatenate([s, c], axis=1)], axis=0)
    )
    en_out[...] = jnp.zeros_like(en_out)
    sum_out[...] = jnp.zeros_like(sum_out)

    def arrive(b):
        for dg, dh in peers:
            tap_copy(b, dg, dh).wait_recv()
            core_copy(b, dg, dh).start()
        if b == 0:
            for dg, dh in peers:
                ser_copy(dg, dh).wait_recv()
        for dg, dh in peers:
            core_copy(b, dg, dh).wait_recv()

    sign = (1 - 2 * g).astype(f32)

    def front(s, b):
        lo, hi = places[b], places[b] + cores * sizes[b]
        for i in range(sub_rows // tile):
            part = pl.ds(i * tile, tile)

            def body(k, carry):
                got = []
                for p in range(n):
                    value = ser[p, s, part] * tap[p, k, part]
                    got.append((value * sign if p % 2 else value, None))
                out = butterfly(got)
                for u in range(half):
                    re, im = out[u]
                    zbuf[u, s, k, 0, part] = re
                    zbuf[u, s, k, 1, part] = out[half][0] if u == 0 else im
                return carry

            lax.fori_loop(lo, hi, body, 0)
        for k in range(lo, hi):
            for part in range(2):
                recv[s, k, part, h] = zbuf[h, s, k, part]

    def z_copy(s, b, dh):
        to = lax.rem(h + dh, half)
        at = pl.ds(places[b], cores * sizes[b])
        return remote(
            zbuf.at[to, s, at], recv.at[s, at, :, h], z_ss.at[s, b, dh], z_rs.at[s, b, dh], friend(dh)
        )

    def z_start(s, b):
        for dh in range(1, half):
            z_copy(s, b, dh).start()

    def en_copy(dh):
        return remote(en_out, en_in.at[dh], en_ss.at[dh], en_rs.at[dh], friend(dh))

    def energy(p, total):
        one, two = tap[p, 0], tap[p, 1]
        new = []
        for s in range(mine):
            a, b = ser[p, s] * one, ser[p, s] * two
            new.append(total[s] + (a * a + b * b))
        return tuple(new)

    arrive(0)
    front(0, 0)
    z_start(0, 0)
    total = lax.fori_loop(0, n, energy, tuple(jnp.zeros((sub_rows, LANES), f32) for _ in range(mine)))
    for s in range(mine):
        en_out[s : s + 1] = jnp.sum(total[s], axis=0, keepdims=True)
    for dh in range(1, half):
        en_copy(dh).start()
    arrive(1)
    front(0, 1)
    z_start(0, 1)
    for s in range(1, mine):
        for b in range(2):
            front(s, b)
        z_start(s, 0)

    for dh in range(1, half):
        en_copy(dh).wait_recv()
    total = en_out[...]
    for dh in range(1, half):
        total += en_in[dh]
    variance0 = [jnp.sum(total[s : s + 1]) * (0.5 / length_all) for s in range(mine)]
    keep = [keep_ref[k] for k in order]

    def sum_copy(it, dh):
        return remote(sum_out.at[it], sum_in.at[it, dh], sum_ss.at[it, dh], sum_rs.at[it, dh], friend(dh))

    def share(it, totals):
        for s, total in enumerate(totals):
            sum_out[it, s : s + 1] = jnp.sum(total, axis=0, keepdims=True)
        for dh in range(1, half):
            sum_copy(it, dh).start()

    def collect(it):
        total = sum_out[it]
        for dh in range(1, half):
            sum_copy(it, dh).wait_recv()
            total += sum_in[it, dh]
        return [jnp.sum(total[s : s + 1]) / length_all for s in range(mine)]

    def transform(s):
        def body(kk, carry):
            k = 2 * kk
            x = jnp.concatenate(
                [recv[s, k].reshape(2 * rows, LANES), recv[s, k + 1].reshape(2 * rows, LANES)], axis=1
            )
            mid = dot3((left[0], left[1]), split(x))
            c, d = inner[0], inner[1]
            turned = []
            for i in range(2):
                lanes = slice(i * LANES, (i + 1) * LANES)
                mr = jnp.concatenate([mid[:rows, lanes], mid[2 * rows :, lanes]], axis=0)
                mi = jnp.concatenate([mid[rows : 2 * rows, lanes], jnp.zeros((extra, LANES), f32)], axis=0)
                turned.append(jnp.concatenate([mr * c + mi * d, mi * c - mr * d], axis=1))
            done = dot3(split(jnp.concatenate(turned, axis=0)), (right[0], right[1]))
            for i in range(2):
                block = done[i * tall : (i + 1) * tall]
                spec[0, k + i] = block[:, :LANES]
                spec[1, k + i] = block[:, LANES:]
            return carry

        lax.fori_loop(0, tapers // 2, body, 0)

    def combine(s, variance):
        def body(i, total):
            at = pl.ds(pl.multiple_of(i * CHUNK, CHUNK), CHUNK)
            re = [spec[0, k, at] for k in range(tapers)]
            im = [spec[1, k, at] for k in range(tapers)]
            sums = [None] * terms
            powers = []
            pair = 0
            for j in range(tapers):
                for k in range(j, tapers):
                    both = re[j] * re[k] + im[j] * im[k]
                    if j == k:
                        powers.append(both)
                        power[s, k, at] = both
                    for t in range(terms):
                        sums[t] = add(sums[t], pairs[t, pair] * both)
                    pair += 1
            for t in range(terms):
                qi[s, t, at] = sums[t]
            new = refine(0.5 * (powers[0] + powers[1]), powers, keep, variance)
            est[s, at] = new
            return total + new * weigh[at]

        return lax.fori_loop(0, tall // CHUNK, body, jnp.zeros((CHUNK, LANES), f32))

    def sweep(s, variance):
        def body(i, total):
            at = pl.ds(pl.multiple_of(i * CHUNK, CHUNK), CHUNK)
            new = refine(est[s, at], [power[s, k, at] for k in range(tapers)], keep, variance)
            est[s, at] = new
            return total + new * weigh[at]

        return lax.fori_loop(0, tall // CHUNK, body, jnp.zeros((CHUNK, LANES), f32))

    def assemble(src):
        mirrored = flip(src[0:rows])

        @pl.when(jnp.logical_not(single))
        def _():
            folded[0] = src[0:rows]
            folded[1] = mirrored

        @pl.when(single)
        def _():
            folded[g, 0 : rows // 2] = src[0 : rows // 2]
            folded[g, rows // 2 : rows // 2 + 1] = src[rows : rows + 1]
            folded[g, rows // 2 + 1 : rows] = mirrored[rows // 2 : rows - 1]
            folded[1 - g, 0 : rows // 2] = mirrored[: rows // 2]
            folded[1 - g, rows // 2 : rows] = src[rows // 2 : rows]

        return folded[0].T, folded[1].T

    def qi_copy(s, t):
        return remote(qi_out.at[s, t], qi_ref.at[g * mine + s, t], qo_ss.at[s, t], qo_rs.at[s, t], partner)

    def spec_copy(s):
        return remote(spec_out.at[s], spec_ref.at[g * mine + s], so_ss.at[s], so_rs.at[s], partner)

    def outputs_qi(s, which):
        for t in which:
            own, sent = assemble(qi.at[s, t])
            qi_ref[g * mine + s, t] = own
            qi_out[s, t] = sent
            qi_copy(s, t).start()

    totals = []
    for s in range(mine):
        for b in range(2):
            for dh in range(1, half):
                z_copy(s, b, dh).wait_recv()
        transform(s)
        totals.append(combine(s, variance0[s]))
        if s < mine - 1:
            outputs_qi(s, range(terms))
            z_start(s + 1, 1)
    for it in range(1, ITERS):
        share(it - 1, totals)
        outputs_qi(mine - 1, range(terms * (it - 1) // (ITERS - 1), terms * it // (ITERS - 1)))
        variance = collect(it - 1)
        totals = [sweep(s, variance[s]) for s in range(mine)]
    for s in range(mine):
        own, sent = assemble(est.at[s])
        spec_ref[g * mine + s] = own
        spec_out[s] = sent
        spec_copy(s).start()

    for s in range(mine):
        for t in range(terms):
            qi_copy(s, t).wait_recv()
        spec_copy(s).wait_recv()
    for s in range(mine):
        for t in range(terms):
            qi_copy(s, t).wait_send()
        spec_copy(s).wait_send()
        for dh in range(1, half):
            for b in range(2):
                z_copy(s, b, dh).wait_send()
    for dh in range(1, half):
        en_copy(dh).wait_send()
        for it in range(ITERS - 1):
            sum_copy(it, dh).wait_send()
    for dg, dh in peers:
        ser_copy(dg, dh).wait_send()
        for b in range(2):
            tap_copy(b, dg, dh).wait_send()
            core_copy(b, dg, dh).wait_send()


def hand_kernel(spec_ref, qi_ref, spec_out, qi_out):
    spec_out[...] = spec_ref[...]
    qi_out[...] = qi_ref[...]


def local(cores, series, tapers, concentration, qi_weights):
    n = lax.axis_size("af")
    count, local_len = series.shape
    taper_count = tapers.shape[0]
    terms = qi_weights.shape[0]
    half, mine = n // 2, count // 2
    sub_rows = local_len // (half * LANES)
    rows = local_len // LANES
    tall = rows + CHUNK
    lead = (taper_count // cores + 1) // 2
    f32 = jnp.float32
    bf16 = jnp.bfloat16
    vmem = pl.BlockSpec(memory_space=pltpu.VMEM)
    smem = pl.BlockSpec(memory_space=pltpu.SMEM)
    dma = pltpu.SemaphoreType.DMA
    shapes = (
        jax.ShapeDtypeStruct((count, LANES, rows), f32),
        jax.ShapeDtypeStruct((count, terms, LANES, rows), f32),
    )
    outs = pl.pallas_call(
        functools.partial(fused_kernel, n, cores, lead),
        out_shape=shapes,
        in_specs=[vmem, vmem, smem, smem],
        out_specs=(vmem, vmem),
        scratch_shapes=[
            pltpu.VMEM((2, 8 * rows, LANES), f32),
            pltpu.VMEM((count, half, sub_rows, LANES), f32),
            pltpu.VMEM((taper_count, half, sub_rows, LANES), f32),
            pltpu.VMEM((n, mine, sub_rows, LANES), f32),
            pltpu.VMEM((n, taper_count, sub_rows, LANES), f32),
            pltpu.VMEM((half, mine, taper_count, 2, sub_rows, LANES), f32),
            pltpu.VMEM((mine, taper_count, 2, half, sub_rows, LANES), f32),
            pltpu.VMEM((8, LANES), f32),
            pltpu.VMEM((half, 8, LANES), f32),
            pltpu.VMEM((ITERS - 1, 8, LANES), f32),
            pltpu.VMEM((ITERS - 1, half, 8, LANES), f32),
            pltpu.VMEM((2, rows + tall, 2 * rows), bf16),
            pltpu.VMEM((2, 2 * LANES, 2 * LANES), bf16),
            pltpu.VMEM((2, tall, LANES), f32),
            pltpu.VMEM((tall, LANES), f32),
            pltpu.VMEM((2, taper_count, tall, LANES), f32),
            pltpu.VMEM((mine, taper_count, tall, LANES), f32),
            pltpu.VMEM((mine, tall, LANES), f32),
            pltpu.VMEM((mine, terms, tall, LANES), f32),
            pltpu.VMEM((mine, LANES, rows), f32),
            pltpu.VMEM((mine, terms, LANES, rows), f32),
            pltpu.SMEM((terms, taper_count * (taper_count + 1) // 2), f32),
            pltpu.VMEM((2, rows, LANES), f32),
            dma((2, half)), dma((2, half)),
            dma((2, 2, half)), dma((2, 2, half)),
            dma((2, 2, half)), dma((2, 2, half)),
            dma((half,)), dma((half,)),
            dma((mine, 2, half)), dma((mine, 2, half)),
            dma((ITERS - 1, half)), dma((ITERS - 1, half)),
            dma((mine, terms)), dma((mine, terms)),
            dma((mine,)), dma((mine,)),
        ],
        compiler_params=pltpu.CompilerParams(collective_id=0, has_side_effects=True),
    )(series, tapers, concentration, qi_weights.transpose(1, 0, 2))
    spectrum, qi_terms = pl.pallas_call(
        hand_kernel, out_shape=shapes, in_specs=[vmem, vmem], out_specs=(vmem, vmem)
    )(*outs)
    return (
        spectrum.reshape(count, 1, local_len),
        qi_terms.reshape(count, terms, 1, local_len),
    )


def solution(mesh):
    placed = (P("sa", "af"), P(None, "af"), P(), P())
    return jax.shard_map(
        functools.partial(local, mesh.shape["sa"]),
        mesh=mesh,
        in_specs=placed,
        out_specs=(P("sa", "af", None), P("sa", None, "af", None)),
        check_vma=False,
    )
```

```python
import functools
import math

import jax
import jax.numpy as jnp
import numpy as np
from jax import lax
from jax.experimental import pallas as pl
from jax.experimental.pallas import tpu as pltpu
from jax.sharding import PartitionSpec as P

ITERS = 3
LANES = 128
CHUNK = 16
MESH = pl.DeviceIdType.MESH


def add(a, b):
    if a is None:
        return b
    return a if b is None else a + b


def sub(a, b):
    if b is None:
        return a
    return -b if a is None else a - b


def butterfly(values):
    n = len(values)
    if n == 1:
        return values
    even, odd = butterfly(values[0::2]), butterfly(values[1::2])
    low, high = [], []
    for k in range(n // 2):
        (er, ei), (tr, ti) = even[k], odd[k]
        if 4 * k == n:
            tr, ti = ti, (None if tr is None else -tr)
        elif k:
            c, s = math.cos(2 * math.pi * k / n), math.sin(2 * math.pi * k / n)
            if ti is None:
                tr, ti = tr * c, tr * (-s)
            else:
                tr, ti = tr * c + ti * s, ti * c - tr * s
        low.append((add(er, tr), add(ei, ti)))
        high.append((sub(er, tr), sub(ei, ti)))
    return low + high


def split(x):
    high = x.astype(jnp.bfloat16)
    return high, (x - high.astype(jnp.float32)).astype(jnp.bfloat16)


def dot3(a, b):
    dot = functools.partial(jnp.dot, preferred_element_type=jnp.float32)
    return dot(a[0], b[0]) + (dot(a[0], b[1]) + dot(a[1], b[0]))


def refine(estimate, powers, keep, variance):
    top = bottom = None
    for k, power in enumerate(powers):
        base = keep[k] * estimate + (1.0 - keep[k]) * variance
        weight = keep[k] / (base * base)
        top = add(top, weight * power)
        bottom = add(bottom, weight)
    return top / bottom


def turn(index, period):
    if period & (period - 1):
        index = lax.rem(index, jnp.full_like(index, period))
    else:
        index = index & (period - 1)
    angle = index.astype(jnp.float32) * (2.0 * math.pi / period)
    return jnp.cos(angle), jnp.sin(angle)


def flip(x):
    rows, lanes = x.shape
    lane = lanes - 1 - lax.broadcasted_iota(jnp.int32, (8, lanes), 1)
    line = 7 - lax.broadcasted_iota(jnp.int32, (8, lanes), 0)
    parts = []
    for i in reversed(range(rows // 8)):
        part = jnp.take_along_axis(x[8 * i : 8 * i + 8], lane, axis=1)
        parts.append(jnp.take_along_axis(part, line, axis=0))
    return jnp.concatenate(parts, axis=0)


def remote(src, dst, send, recv, where):
    return pltpu.make_async_remote_copy(
        src_ref=src, dst_ref=dst, send_sem=send, recv_sem=recv, device_id=where, device_id_type=MESH
    )


def fused_kernel(
    n, cores, sizes, series_hbm, tapers_hbm, keep_ref, mix_ref, spec_ref, qi_ref,
    series_ref, tapers_ref, stage, ser_src, tap_src, ser, tap, zbuf, recv, en_out, en_in, sum_out, sum_in, left, right, inner, weigh,
    spec, power, est, qi, spec_out, qi_out, pairs, folded,
    ser_ss, ser_rs, tap_ss, tap_rs, core_ss, core_rs, en_ss, en_rs, z_ss, z_rs,
    sum_ss, sum_rs, qo_ss, qo_rs, so_ss, so_rs, in_sem,
):
    inputs = [
        pltpu.make_async_copy(series_hbm, series_ref, in_sem.at[0]),
        pltpu.make_async_copy(tapers_hbm, tapers_ref, in_sem.at[1]),
    ]
    for copy in inputs:
        copy.start()
    half = n // 2
    count, sub_rows = ser_src.shape[0], ser_src.shape[2]
    mine = count // 2
    tapers, terms = tap.shape[1], mix_ref.shape[1]
    group = tapers // cores
    batches = range(len(sizes))
    starts = [sum(sizes[:b]) for b in batches]
    places = [cores * start for start in starts]
    order = [c * group + starts[b] + i for b in batches for c in range(cores) for i in range(sizes[b])]
    early = [order.index(0), order.index(1)]
    rows = half * sub_rows
    tall = spec.shape[2]
    extra = tall - rows
    local_len = rows * LANES
    length_all = local_len * n
    tile = min(8, sub_rows)
    f32 = jnp.float32
    me, core = lax.axis_index("af"), lax.axis_index("sa")
    g, h = me // half, lax.rem(me, half)
    peers = [(dg, dh) for dg in (0, 1) for dh in range(half) if dg or dh]
    single = h == 0

    def ahead(dg, dh):
        return lax.rem(g + dg, 2), lax.rem(h + dh, half)

    def flat(at):
        return at[0] * half + at[1]

    def friend(dh):
        return {"af": g * half + lax.rem(h + dh, half)}

    partner = {"af": (1 - g) * half + lax.rem(half - h, half)}
    other_core = lax.rem(core + 1, cores)

    barrier = pltpu.get_barrier_semaphore()
    for dg, dh in peers:
        pl.semaphore_signal(barrier, inc=1, device_id={"af": flat(ahead(dg, dh))}, device_id_type=MESH)
    pl.semaphore_signal(barrier, inc=1, device_id={"sa": other_core}, device_id_type=MESH)

    for copy in inputs:
        copy.wait()
    for j in range(rows):
        lanes = slice(j * LANES, (j + 1) * LANES)
        stage[0, 8 * j : 8 * j + 8] = tapers_ref[0:8, lanes]
        stage[1, 8 * j : 8 * j + tapers - 8] = tapers_ref[8:tapers, lanes]
        stage[1, 8 * j + tapers - 8 : 8 * j + tapers - 8 + count] = series_ref[:, lanes]
    for row in range(tapers + count):
        for j in range(rows // tile):
            part = stage[row // 8, pl.ds(8 * j * tile + row % 8, tile, stride=8)]
            at = (j * tile // sub_rows, slice(j * tile % sub_rows, j * tile % sub_rows + tile))
            if row < tapers:
                tap_src[row, at[0], at[1]] = part
            else:
                ser_src[row - tapers, at[0], at[1]] = part
    pl.semaphore_wait(barrier, n)

    def ser_copy(dg, dh):
        to = ahead(dg, dh)
        return remote(
            ser_src.at[pl.ds(to[0] * mine, mine), to[1]], ser.at[me],
            ser_ss.at[0], ser_rs.at[0], {"af": flat(to)},
        )

    def tap_copy(b, dg, dh):
        to = ahead(dg, dh)
        return remote(
            tap_src.at[pl.ds(core * group + starts[b], sizes[b]), to[1]],
            tap.at[me, pl.ds(places[b] + core * sizes[b], sizes[b])],
            tap_ss.at[b], tap_rs.at[b], {"af": flat(to)},
        )

    def core_copy(b):
        at = tap.at[:, pl.ds(places[b] + core * sizes[b], sizes[b])]
        return remote(at, at, core_ss.at[b], core_rs.at[b], {"sa": other_core})

    def settle(like, semaphore):
        pltpu.make_async_copy(like, like, semaphore).wait()

    ser_like = ser.at[pl.ds(0, n - 1)]
    tap_like = [tap.at[pl.ds(0, n - 1), pl.ds(places[b], sizes[b])] for b in batches]
    z_like = [
        [recv.at[s, pl.ds(places[b], cores * sizes[b]), :, pl.ds(0, half - 1)] for b in batches]
        for s in range(mine)
    ]
    en_like = en_in.at[pl.ds(1, half - 1)]
    sum_like = [sum_in.at[it, pl.ds(1, half - 1)] for it in range(ITERS - 1)]

    for b in batches:
        for dg, dh in peers:
            if b == 0:
                ser_copy(dg, dh).start()
            tap_copy(b, dg, dh).start()

    for s in range(mine):
        ser[me, s] = ser_src[g * mine + s, h]
    for b in batches:
        for i in range(sizes[b]):
            tap[me, places[b] + core * sizes[b] + i] = tap_src[core * group + starts[b] + i, h]
    for t in range(terms):
        p = 0
        for j in range(tapers):
            for k in range(j, tapers):
                value = mix_ref[order[j], t, order[k]]
                pairs[t, p] = value if j == k else value + mix_ref[order[k], t, order[j]]
                p += 1

    def frequency(shape):
        at = lax.broadcasted_iota(jnp.int32, shape, 0)
        upper = (at >= rows // 2) & (at < rows)
        class_of = jnp.where(single, jnp.where(upper, half, 0), me)
        line = jnp.where(at < rows, at, rows // 2)
        class_of = jnp.where(at < rows, class_of, 0)
        return n * line + class_of, at, upper

    freq, at, upper = frequency((tall, rows))
    c, s = turn(lax.broadcasted_iota(jnp.int32, (tall, rows), 1) * freq, rows * n)
    first = jnp.where(upper, 1, 0) == g
    inside = at < rows
    once = at == rows
    take0 = jnp.where(single, jnp.where(inside | once, jnp.where(first, 1.0, 0.0), 0.0), jnp.where(inside, 1.0, 0.0))
    take1 = jnp.where(single, jnp.where(inside | once, jnp.where(first, 0.0, 1.0), 0.0), 0.0)
    plain = jnp.where(single, 0.0, jnp.where(inside, 1.0, 0.0))
    real0, real1 = c * take0, c * take1 + s * plain
    imag0, imag1 = -(s * take0), c * plain - s * take1
    full = jnp.concatenate(
        [
            jnp.concatenate([real0[:rows], real1[:rows]], axis=1),
            jnp.concatenate([imag0[:rows], imag1[:rows]], axis=1),
            jnp.concatenate([real0[rows:], real1[rows:]], axis=1),
        ],
        axis=0,
    )
    left[0], left[1] = split(full)

    freq, at, upper = frequency((tall, LANES))
    c, s = turn(lax.broadcasted_iota(jnp.int32, (tall, LANES), 1) * freq, length_all)
    scale = 1.0 / math.sqrt(length_all)
    inner[0], inner[1] = c * scale, s * scale
    weigh[...] = jnp.where(
        single,
        jnp.where(at < rows, jnp.where(at == 0, 1.0, 2.0), jnp.where(at == rows, 1.0, 0.0)),
        jnp.where(at < rows, 2.0, 0.0),
    )
    grid = (LANES, LANES)
    c, s = turn(lax.broadcasted_iota(jnp.int32, grid, 0) * lax.broadcasted_iota(jnp.int32, grid, 1), LANES)
    right[0], right[1] = split(
        jnp.concatenate([jnp.concatenate([c, -s], axis=1), jnp.concatenate([s, c], axis=1)], axis=0)
    )
    en_out[...] = jnp.zeros_like(en_out)
    sum_out[...] = jnp.zeros_like(sum_out)

    def arrive(b):
        settle(tap_like[b], tap_rs.at[b])
        core_copy(b).start()
        if b == 0:
            settle(ser_like, ser_rs.at[0])
        core_copy(b).wait_recv()

    sign = (1 - 2 * g).astype(f32)

    def front(s, b):
        lo, hi = places[b], places[b] + cores * sizes[b]
        for i in range(sub_rows // tile):
            part = pl.ds(i * tile, tile)

            def body(k, carry):
                got = []
                for p in range(n):
                    value = ser[p, s, part] * tap[p, k, part]
                    got.append((value * sign if p % 2 else value, None))
                out = butterfly(got)
                for u in range(half):
                    re, im = out[u]
                    zbuf[u, s, k, 0, part] = re
                    zbuf[u, s, k, 1, part] = out[half][0] if u == 0 else im
                return carry

            lax.fori_loop(lo, hi, body, 0)
        for k in range(lo, hi):
            for part in range(2):
                recv[s, k, part, h] = zbuf[h, s, k, part]

    def z_copy(s, b, dh):
        to = lax.rem(h + dh, half)
        at = pl.ds(places[b], cores * sizes[b])
        return remote(
            zbuf.at[to, s, at], recv.at[s, at, :, h], z_ss.at[s, b], z_rs.at[s, b], friend(dh)
        )

    def z_start(s, b):
        for dh in range(1, half):
            z_copy(s, b, dh).start()

    def en_copy(dh):
        return remote(en_out, en_in.at[dh], en_ss.at[0], en_rs.at[0], friend(dh))

    def energy(p, total):
        one, two = tap[p, early[0]], tap[p, early[1]]
        new = []
        for s in range(mine):
            a, b = ser[p, s] * one, ser[p, s] * two
            new.append(total[s] + (a * a + b * b))
        return tuple(new)

    for b in batches:
        arrive(b)
        front(0, b)
        z_start(0, b)
        if max(early) < places[b] + cores * sizes[b] and max(early) >= places[b]:
            total = lax.fori_loop(0, n, energy, tuple(jnp.zeros((sub_rows, LANES), f32) for _ in range(mine)))
            for s in range(mine):
                en_out[s : s + 1] = jnp.sum(total[s], axis=0, keepdims=True)
            for dh in range(1, half):
                en_copy(dh).start()
    for s in range(1, mine):
        for b in batches:
            front(s, b)
            z_start(s, b)

    settle(ser_like, ser_ss.at[0])
    for b in batches:
        settle(tap_like[b], tap_ss.at[b])
        core_copy(b).wait_send()

    def first_variance():
        settle(en_like, en_rs.at[0])
        settle(en_like, en_ss.at[0])
        total = en_out[...]
        for dh in range(1, half):
            total += en_in[dh]
        return [jnp.sum(total[s : s + 1]) * (0.5 / length_all) for s in range(mine)]

    keep = [keep_ref[k] for k in order]

    def sum_copy(it, dh):
        return remote(sum_out.at[it], sum_in.at[it, dh], sum_ss.at[it], sum_rs.at[it], friend(dh))

    def share(it, totals):
        for s, total in enumerate(totals):
            sum_out[it, s : s + 1] = jnp.sum(total, axis=0, keepdims=True)
        for dh in range(1, half):
            sum_copy(it, dh).start()

    def collect(it):
        settle(sum_like[it], sum_rs.at[it])
        total = sum_out[it]
        for dh in range(1, half):
            total += sum_in[it, dh]
        return [jnp.sum(total[s : s + 1]) / length_all for s in range(mine)]

    def transform(s, b):
        def body(kk, carry):
            k = 2 * kk
            x = jnp.concatenate(
                [recv[s, k].reshape(2 * rows, LANES), recv[s, k + 1].reshape(2 * rows, LANES)], axis=1
            )
            mid = dot3((left[0], left[1]), split(x))
            c, d = inner[0], inner[1]
            turned = []
            for i in range(2):
                lanes = slice(i * LANES, (i + 1) * LANES)
                mr = jnp.concatenate([mid[:rows, lanes], mid[2 * rows :, lanes]], axis=0)
                mi = jnp.concatenate([mid[rows : 2 * rows, lanes], jnp.zeros((extra, LANES), f32)], axis=0)
                turned.append(jnp.concatenate([mr * c + mi * d, mi * c - mr * d], axis=1))
            done = dot3(split(jnp.concatenate(turned, axis=0)), (right[0], right[1]))
            for i in range(2):
                block = done[i * tall : (i + 1) * tall]
                spec[0, k + i] = block[:, :LANES]
                spec[1, k + i] = block[:, LANES:]
            return carry

        lax.fori_loop(places[b] // 2, (places[b] + cores * sizes[b]) // 2, body, 0)

    def combine(s, variance):
        def body(i, total):
            at = pl.ds(pl.multiple_of(i * CHUNK, CHUNK), CHUNK)
            re = [spec[0, k, at] for k in range(tapers)]
            im = [spec[1, k, at] for k in range(tapers)]
            sums = [None] * terms
            powers = []
            pair = 0
            for j in range(tapers):
                for k in range(j, tapers):
                    both = re[j] * re[k] + im[j] * im[k]
                    if j == k:
                        powers.append(both)
                        power[s, k, at] = both
                    for t in range(terms):
                        sums[t] = add(sums[t], pairs[t, pair] * both)
                    pair += 1
            for t in range(terms):
                qi[s, t, at] = sums[t]
            new = refine(0.5 * (powers[early[0]] + powers[early[1]]), powers, keep, variance)
            est[s, at] = new
            return total + new * weigh[at]

        return lax.fori_loop(0, tall // CHUNK, body, jnp.zeros((CHUNK, LANES), f32))

    def sweep(s, variance):
        def body(i, total):
            at = pl.ds(pl.multiple_of(i * CHUNK, CHUNK), CHUNK)
            new = refine(est[s, at], [power[s, k, at] for k in range(tapers)], keep, variance)
            est[s, at] = new
            return total + new * weigh[at]

        return lax.fori_loop(0, tall // CHUNK, body, jnp.zeros((CHUNK, LANES), f32))

    def assemble(src):
        mirrored = flip(src[0:rows])

        @pl.when(jnp.logical_not(single))
        def _():
            folded[0] = src[0:rows]
            folded[1] = mirrored

        @pl.when(single)
        def _():
            folded[g, 0 : rows // 2] = src[0 : rows // 2]
            folded[g, rows // 2 : rows // 2 + 1] = src[rows : rows + 1]
            folded[g, rows // 2 + 1 : rows] = mirrored[rows // 2 : rows - 1]
            folded[1 - g, 0 : rows // 2] = mirrored[: rows // 2]
            folded[1 - g, rows // 2 : rows] = src[rows // 2 : rows]

        return folded[0].T, folded[1].T

    def qi_copy(s, t):
        return remote(qi_out.at[s, t], qi_ref.at[g * mine + s, t], qo_ss.at[s], qo_rs.at[s], partner)

    def spec_copy(s):
        return remote(spec_out.at[s], spec_ref.at[g * mine + s], so_ss.at[0], so_rs.at[0], partner)

    def outputs_qi(s, which):
        for t in which:
            own, sent = assemble(qi.at[s, t])
            qi_ref[g * mine + s, t] = own
            qi_out[s, t] = sent
            qi_copy(s, t).start()

    totals = []
    for s in range(mine):
        for b in batches:
            settle(z_like[s][b], z_rs.at[s, b])
            transform(s, b)
        if s == 0:
            variance0 = first_variance()
        totals.append(combine(s, variance0[s]))
        if s < mine - 1:
            outputs_qi(s, range(terms))
    for it in range(1, ITERS):
        share(it - 1, totals)
        outputs_qi(mine - 1, range(terms * (it - 1) // (ITERS - 1), terms * it // (ITERS - 1)))
        variance = collect(it - 1)
        totals = [sweep(s, variance[s]) for s in range(mine)]
    for s in range(mine):
        own, sent = assemble(est.at[s])
        spec_ref[g * mine + s] = own
        spec_out[s] = sent
        spec_copy(s).start()

    for s in range(mine):
        for b in batches:
            settle(z_like[s][b], z_ss.at[s, b])
    for it in range(ITERS - 1):
        settle(sum_like[it], sum_ss.at[it])
    for s in range(mine):
        settle(qi_out.at[s], qo_rs.at[s])
        settle(qi_out.at[s], qo_ss.at[s])
    settle(spec_out, so_rs.at[0])
    settle(spec_out, so_ss.at[0])


def hand_kernel(spec_ref, qi_ref, spec_out, qi_out):
    spec_out[...] = spec_ref[...]
    qi_out[...] = qi_ref[...]


def local(cores, series, tapers, concentration, qi_weights):
    n = lax.axis_size("af")
    count, local_len = series.shape
    taper_count = tapers.shape[0]
    terms = qi_weights.shape[0]
    half, mine = n // 2, count // 2
    sub_rows = local_len // (half * LANES)
    rows = local_len // LANES
    tall = rows + CHUNK
    sizes = (1,) * (taper_count // cores)
    f32 = jnp.float32
    bf16 = jnp.bfloat16
    vmem = pl.BlockSpec(memory_space=pltpu.VMEM)
    smem = pl.BlockSpec(memory_space=pltpu.SMEM)
    hbm = pl.BlockSpec(memory_space=pltpu.HBM)
    dma = pltpu.SemaphoreType.DMA
    shapes = (
        jax.ShapeDtypeStruct((count, LANES, rows), f32),
        jax.ShapeDtypeStruct((count, terms, LANES, rows), f32),
    )
    outs = pl.pallas_call(
        functools.partial(fused_kernel, n, cores, sizes),
        out_shape=shapes,
        in_specs=[hbm, hbm, smem, smem],
        out_specs=(vmem, vmem),
        scratch_shapes=[
            pltpu.VMEM(series.shape, f32),
            pltpu.VMEM(tapers.shape, f32),
            pltpu.VMEM((2, 8 * rows, LANES), f32),
            pltpu.VMEM((count, half, sub_rows, LANES), f32),
            pltpu.VMEM((taper_count, half, sub_rows, LANES), f32),
            pltpu.VMEM((n, mine, sub_rows, LANES), f32),
            pltpu.VMEM((n, taper_count, sub_rows, LANES), f32),
            pltpu.VMEM((half, mine, taper_count, 2, sub_rows, LANES), f32),
            pltpu.VMEM((mine, taper_count, 2, half, sub_rows, LANES), f32),
            pltpu.VMEM((8, LANES), f32),
            pltpu.VMEM((half, 8, LANES), f32),
            pltpu.VMEM((ITERS - 1, 8, LANES), f32),
            pltpu.VMEM((ITERS - 1, half, 8, LANES), f32),
            pltpu.VMEM((2, rows + tall, 2 * rows), bf16),
            pltpu.VMEM((2, 2 * LANES, 2 * LANES), bf16),
            pltpu.VMEM((2, tall, LANES), f32),
            pltpu.VMEM((tall, LANES), f32),
            pltpu.VMEM((2, taper_count, tall, LANES), f32),
            pltpu.VMEM((mine, taper_count, tall, LANES), f32),
            pltpu.VMEM((mine, tall, LANES), f32),
            pltpu.VMEM((mine, terms, tall, LANES), f32),
            pltpu.VMEM((mine, LANES, rows), f32),
            pltpu.VMEM((mine, terms, LANES, rows), f32),
            pltpu.SMEM((terms, taper_count * (taper_count + 1) // 2), f32),
            pltpu.VMEM((2, rows, LANES), f32),
            dma((1,)), dma((1,)),
            dma((len(sizes),)), dma((len(sizes),)),
            dma((len(sizes),)), dma((len(sizes),)),
            dma((1,)), dma((1,)),
            dma((mine, len(sizes))), dma((mine, len(sizes))),
            dma((ITERS - 1,)), dma((ITERS - 1,)),
            dma((mine,)), dma((mine,)),
            dma((1,)), dma((1,)),
            dma((2,)),
        ],
        compiler_params=pltpu.CompilerParams(collective_id=0, has_side_effects=True),
    )(series, tapers, concentration, qi_weights.transpose(1, 0, 2))
    spectrum, qi_terms = pl.pallas_call(
        hand_kernel, out_shape=shapes, in_specs=[vmem, vmem], out_specs=(vmem, vmem)
    )(*outs)
    return (
        spectrum.reshape(count, 1, local_len),
        qi_terms.reshape(count, terms, 1, local_len),
    )


def solution(mesh):
    placed = (P("sa", "af"), P(None, "af"), P(), P())
    return jax.shard_map(
        functools.partial(local, mesh.shape["sa"]),
        mesh=mesh,
        in_specs=placed,
        out_specs=(P("sa", "af", None), P("sa", None, "af", None)),
        check_vma=False,
    )
```

```python
import functools
import math

import jax
import jax.numpy as jnp
import numpy as np
from jax import lax
from jax.experimental import pallas as pl
from jax.experimental.pallas import tpu as pltpu
from jax.sharding import PartitionSpec as P

ITERS = 3
LANES = 128
CHUNK = 16
MESH = pl.DeviceIdType.MESH


def add(a, b):
    if a is None:
        return b
    return a if b is None else a + b


def sub(a, b):
    if b is None:
        return a
    return -b if a is None else a - b


def butterfly(values):
    n = len(values)
    if n == 1:
        return values
    even, odd = butterfly(values[0::2]), butterfly(values[1::2])
    low, high = [], []
    for k in range(n // 2):
        (er, ei), (tr, ti) = even[k], odd[k]
        if 4 * k == n:
            tr, ti = ti, (None if tr is None else -tr)
        elif k:
            c, s = math.cos(2 * math.pi * k / n), math.sin(2 * math.pi * k / n)
            if ti is None:
                tr, ti = tr * c, tr * (-s)
            else:
                tr, ti = tr * c + ti * s, ti * c - tr * s
        low.append((add(er, tr), add(ei, ti)))
        high.append((sub(er, tr), sub(ei, ti)))
    return low + high


def split(x):
    high = x.astype(jnp.bfloat16)
    return high, (x - high.astype(jnp.float32)).astype(jnp.bfloat16)


def dot3(a, b):
    dot = functools.partial(jnp.dot, preferred_element_type=jnp.float32)
    return dot(a[0], b[0]) + (dot(a[0], b[1]) + dot(a[1], b[0]))


def refine(estimate, powers, keep, variance):
    top = bottom = None
    for k, power in enumerate(powers):
        base = keep[k] * estimate + (1.0 - keep[k]) * variance
        weight = keep[k] / (base * base)
        top = add(top, weight * power)
        bottom = add(bottom, weight)
    return top / bottom


def turn(index, period):
    if period & (period - 1):
        index = lax.rem(index, jnp.full_like(index, period))
    else:
        index = index & (period - 1)
    angle = index.astype(jnp.float32) * (2.0 * math.pi / period)
    return jnp.cos(angle), jnp.sin(angle)


def flip(x):
    rows, lanes = x.shape
    lane = lanes - 1 - lax.broadcasted_iota(jnp.int32, (8, lanes), 1)
    line = 7 - lax.broadcasted_iota(jnp.int32, (8, lanes), 0)
    parts = []
    for i in reversed(range(rows // 8)):
        part = jnp.take_along_axis(x[8 * i : 8 * i + 8], lane, axis=1)
        parts.append(jnp.take_along_axis(part, line, axis=0))
    return jnp.concatenate(parts, axis=0)


def remote(src, dst, send, recv, where):
    return pltpu.make_async_remote_copy(
        src_ref=src, dst_ref=dst, send_sem=send, recv_sem=recv, device_id=where, device_id_type=MESH
    )


def fused_kernel(
    n, cores, sizes, series_hbm, tapers_hbm, keep_ref, mix_ref, spec_ref, qi_ref,
    series_ref, tapers_ref, stage, ser_src, tap_src, ser, tap, zbuf, recv, en_out, en_in, sum_out, sum_in, left, right, inner, weigh,
    spec, power, est, qi, spec_out, qi_out, spec_own, qi_own, pairs, folded,
    ser_ss, ser_rs, tap_ss, tap_rs, core_ss, core_rs, en_ss, en_rs, z_ss, z_rs,
    sum_ss, sum_rs, qo_ss, qo_rs, so_ss, so_rs, in_sem, own_sem,
):
    inputs = [
        pltpu.make_async_copy(series_hbm, series_ref, in_sem.at[0]),
        pltpu.make_async_copy(tapers_hbm, tapers_ref, in_sem.at[1]),
    ]
    for copy in inputs:
        copy.start()
    half = n // 2
    count, sub_rows = ser_src.shape[0], ser_src.shape[2]
    mine = count // 2
    tapers, terms = tap.shape[1], mix_ref.shape[1]
    group = tapers // cores
    batches = range(len(sizes))
    starts = [sum(sizes[:b]) for b in batches]
    places = [cores * start for start in starts]
    order = [c * group + starts[b] + i for b in batches for c in range(cores) for i in range(sizes[b])]
    early = [order.index(0), order.index(1)]
    rows = half * sub_rows
    tall = spec.shape[2]
    extra = tall - rows
    local_len = rows * LANES
    length_all = local_len * n
    tile = min(8, sub_rows)
    f32 = jnp.float32
    me, core = lax.axis_index("af"), lax.axis_index("sa")
    g, h = me // half, lax.rem(me, half)
    peers = [(dg, dh) for dg in (0, 1) for dh in range(half) if dg or dh]
    single = h == 0

    def ahead(dg, dh):
        return lax.rem(g + dg, 2), lax.rem(h + dh, half)

    def flat(at):
        return at[0] * half + at[1]

    def friend(dh):
        return {"af": g * half + lax.rem(h + dh, half)}

    partner = {"af": (1 - g) * half + lax.rem(half - h, half)}
    other_core = lax.rem(core + 1, cores)

    barrier = pltpu.get_barrier_semaphore()
    for dg, dh in peers:
        pl.semaphore_signal(barrier, inc=1, device_id={"af": flat(ahead(dg, dh))}, device_id_type=MESH)
    pl.semaphore_signal(barrier, inc=1, device_id={"sa": other_core}, device_id_type=MESH)

    for copy in inputs:
        copy.wait()
    for j in range(rows):
        lanes = slice(j * LANES, (j + 1) * LANES)
        stage[0, 8 * j : 8 * j + 8] = tapers_ref[0:8, lanes]
        stage[1, 8 * j : 8 * j + tapers - 8] = tapers_ref[8:tapers, lanes]
        stage[1, 8 * j + tapers - 8 : 8 * j + tapers - 8 + count] = series_ref[:, lanes]
    for row in range(tapers + count):
        for j in range(rows // tile):
            part = stage[row // 8, pl.ds(8 * j * tile + row % 8, tile, stride=8)]
            at = (j * tile // sub_rows, slice(j * tile % sub_rows, j * tile % sub_rows + tile))
            if row < tapers:
                tap_src[row, at[0], at[1]] = part
            else:
                ser_src[row - tapers, at[0], at[1]] = part
    pl.semaphore_wait(barrier, n)

    def ser_copy(s, dg, dh):
        to = ahead(dg, dh)
        return remote(
            ser_src.at[to[0] * mine + s, to[1]], ser.at[s, me], ser_ss.at[s], ser_rs.at[s], {"af": flat(to)}
        )

    def tap_copy(b, dg, dh):
        to = ahead(dg, dh)
        return remote(
            tap_src.at[pl.ds(core * group + starts[b], sizes[b]), to[1]],
            tap.at[me, pl.ds(places[b] + core * sizes[b], sizes[b])],
            tap_ss.at[b], tap_rs.at[b], {"af": flat(to)},
        )

    def core_copy(b):
        at = tap.at[:, pl.ds(places[b] + core * sizes[b], sizes[b])]
        return remote(at, at, core_ss.at[b], core_rs.at[b], {"sa": other_core})

    def settle(like, semaphore):
        pltpu.make_async_copy(like, like, semaphore).wait()

    ser_like = [ser.at[s, pl.ds(0, n - 1)] for s in range(mine)]
    carried = [[s for s in range(mine) if (0 if s == 0 else len(sizes) - 1) == b] for b in batches]
    tap_like = [tap.at[pl.ds(0, n - 1), pl.ds(places[b], sizes[b])] for b in batches]
    z_like = [
        [recv.at[s, pl.ds(places[b], cores * sizes[b]), :, pl.ds(0, half - 1)] for b in batches]
        for s in range(mine)
    ]
    en_like = en_in.at[pl.ds(1, half - 1)]
    sum_like = [sum_in.at[it, pl.ds(1, half - 1)] for it in range(ITERS - 1)]

    for b in batches:
        for dg, dh in peers:
            for s in carried[b]:
                ser_copy(s, dg, dh).start()
            tap_copy(b, dg, dh).start()

    for s in range(mine):
        ser[s, me] = ser_src[g * mine + s, h]
    for b in batches:
        for i in range(sizes[b]):
            tap[me, places[b] + core * sizes[b] + i] = tap_src[core * group + starts[b] + i, h]
    for t in range(terms):
        p = 0
        for j in range(tapers):
            for k in range(j, tapers):
                value = mix_ref[order[j], t, order[k]]
                pairs[t, p] = value if j == k else value + mix_ref[order[k], t, order[j]]
                p += 1

    def frequency(shape):
        at = lax.broadcasted_iota(jnp.int32, shape, 0)
        upper = (at >= rows // 2) & (at < rows)
        class_of = jnp.where(single, jnp.where(upper, half, 0), me)
        line = jnp.where(at < rows, at, rows // 2)
        class_of = jnp.where(at < rows, class_of, 0)
        return n * line + class_of, at, upper

    freq, at, upper = frequency((tall, rows))
    c, s = turn(lax.broadcasted_iota(jnp.int32, (tall, rows), 1) * freq, rows * n)
    first = jnp.where(upper, 1, 0) == g
    inside = at < rows
    once = at == rows
    take0 = jnp.where(single, jnp.where(inside | once, jnp.where(first, 1.0, 0.0), 0.0), jnp.where(inside, 1.0, 0.0))
    take1 = jnp.where(single, jnp.where(inside | once, jnp.where(first, 0.0, 1.0), 0.0), 0.0)
    plain = jnp.where(single, 0.0, jnp.where(inside, 1.0, 0.0))
    real0, real1 = c * take0, c * take1 + s * plain
    imag0, imag1 = -(s * take0), c * plain - s * take1
    full = jnp.concatenate(
        [
            jnp.concatenate([real0[:rows], real1[:rows]], axis=1),
            jnp.concatenate([imag0[:rows], imag1[:rows]], axis=1),
            jnp.concatenate([real0[rows:], real1[rows:]], axis=1),
        ],
        axis=0,
    )
    left[0], left[1] = split(full)

    freq, at, upper = frequency((tall, LANES))
    c, s = turn(lax.broadcasted_iota(jnp.int32, (tall, LANES), 1) * freq, length_all)
    scale = 1.0 / math.sqrt(length_all)
    inner[0], inner[1] = c * scale, s * scale
    weigh[...] = jnp.where(
        single,
        jnp.where(at < rows, jnp.where(at == 0, 1.0, 2.0), jnp.where(at == rows, 1.0, 0.0)),
        jnp.where(at < rows, 2.0, 0.0),
    )
    grid = (LANES, LANES)
    c, s = turn(lax.broadcasted_iota(jnp.int32, grid, 0) * lax.broadcasted_iota(jnp.int32, grid, 1), LANES)
    right[0], right[1] = split(
        jnp.concatenate([jnp.concatenate([c, -s], axis=1), jnp.concatenate([s, c], axis=1)], axis=0)
    )
    en_out[...] = jnp.zeros_like(en_out)
    sum_out[...] = jnp.zeros_like(sum_out)

    def arrive(b):
        settle(tap_like[b], tap_rs.at[b])
        core_copy(b).start()
        for s in carried[b]:
            settle(ser_like[s], ser_rs.at[s])
        core_copy(b).wait_recv()

    sign = (1 - 2 * g).astype(f32)

    def front(s, b):
        lo, hi = places[b], places[b] + cores * sizes[b]
        for i in range(sub_rows // tile):
            part = pl.ds(i * tile, tile)

            def body(k, carry):
                got = []
                for p in range(n):
                    value = ser[s, p, part] * tap[p, k, part]
                    got.append((value * sign if p % 2 else value, None))
                out = butterfly(got)
                for u in range(half):
                    re, im = out[u]
                    zbuf[u, s, k, 0, part] = re
                    zbuf[u, s, k, 1, part] = out[half][0] if u == 0 else im
                return carry

            lax.fori_loop(lo, hi, body, 0)
        for k in range(lo, hi):
            for part in range(2):
                recv[s, k, part, h] = zbuf[h, s, k, part]

    def z_copy(s, b, dh):
        to = lax.rem(h + dh, half)
        at = pl.ds(places[b], cores * sizes[b])
        return remote(
            zbuf.at[to, s, at], recv.at[s, at, :, h], z_ss.at[s, b], z_rs.at[s, b], friend(dh)
        )

    def z_start(s, b):
        for dh in range(1, half):
            z_copy(s, b, dh).start()

    def en_copy(dh):
        return remote(en_out, en_in.at[dh], en_ss.at[0], en_rs.at[0], friend(dh))

    def energy(p, total):
        one, two = tap[p, early[0]], tap[p, early[1]]
        new = []
        for s in range(mine):
            a, b = ser[s, p] * one, ser[s, p] * two
            new.append(total[s] + (a * a + b * b))
        return tuple(new)

    for b in batches:
        arrive(b)
        front(0, b)
        if b == len(sizes) - 1:
            total = lax.fori_loop(0, n, energy, tuple(jnp.zeros((sub_rows, LANES), f32) for _ in range(mine)))
            for s in range(mine):
                en_out[s : s + 1] = jnp.sum(total[s], axis=0, keepdims=True)
            for dh in range(1, half):
                en_copy(dh).start()
        z_start(0, b)
    for s in range(1, mine):
        for b in batches:
            front(s, b)
            z_start(s, b)

    for s in range(mine):
        settle(ser_like[s], ser_ss.at[s])
    for b in batches:
        settle(tap_like[b], tap_ss.at[b])
        core_copy(b).wait_send()

    def first_variance():
        settle(en_like, en_rs.at[0])
        settle(en_like, en_ss.at[0])
        total = en_out[...]
        for dh in range(1, half):
            total += en_in[dh]
        return [jnp.sum(total[s : s + 1]) * (0.5 / length_all) for s in range(mine)]

    keep = [keep_ref[k] for k in order]

    def sum_copy(it, dh):
        return remote(sum_out.at[it], sum_in.at[it, dh], sum_ss.at[it], sum_rs.at[it], friend(dh))

    def share(it, totals):
        for s, total in enumerate(totals):
            sum_out[it, s : s + 1] = jnp.sum(total, axis=0, keepdims=True)
        for dh in range(1, half):
            sum_copy(it, dh).start()

    def collect(it):
        settle(sum_like[it], sum_rs.at[it])
        total = sum_out[it]
        for dh in range(1, half):
            total += sum_in[it, dh]
        return [jnp.sum(total[s : s + 1]) / length_all for s in range(mine)]

    def transform(s, b):
        def body(kk, carry):
            k = 2 * kk
            x = jnp.concatenate(
                [recv[s, k].reshape(2 * rows, LANES), recv[s, k + 1].reshape(2 * rows, LANES)], axis=1
            )
            mid = dot3((left[0], left[1]), split(x))
            c, d = inner[0], inner[1]
            turned = []
            for i in range(2):
                lanes = slice(i * LANES, (i + 1) * LANES)
                mr = jnp.concatenate([mid[:rows, lanes], mid[2 * rows :, lanes]], axis=0)
                mi = jnp.concatenate([mid[rows : 2 * rows, lanes], jnp.zeros((extra, LANES), f32)], axis=0)
                turned.append(jnp.concatenate([mr * c + mi * d, mi * c - mr * d], axis=1))
            done = dot3(split(jnp.concatenate(turned, axis=0)), (right[0], right[1]))
            for i in range(2):
                block = done[i * tall : (i + 1) * tall]
                spec[0, k + i] = block[:, :LANES]
                spec[1, k + i] = block[:, LANES:]
            return carry

        lax.fori_loop(places[b] // 2, (places[b] + cores * sizes[b]) // 2, body, 0)

    def measure(s, variance):
        def body(i, total):
            at = pl.ds(pl.multiple_of(i * CHUNK, CHUNK), CHUNK)
            powers = []
            for k in range(tapers):
                re, im = spec[0, k, at], spec[1, k, at]
                powers.append(re * re + im * im)
                power[s, k, at] = powers[k]
            new = refine(0.5 * (powers[early[0]] + powers[early[1]]), powers, keep, variance)
            est[s, at] = new
            return total + new * weigh[at]

        return lax.fori_loop(0, tall // CHUNK, body, jnp.zeros((CHUNK, LANES), f32))

    def combine(s):
        def body(i, carry):
            at = pl.ds(pl.multiple_of(i * CHUNK, CHUNK), CHUNK)
            re = [spec[0, k, at] for k in range(tapers)]
            im = [spec[1, k, at] for k in range(tapers)]
            sums = [None] * terms
            pair = 0
            for j in range(tapers):
                for k in range(j, tapers):
                    both = power[s, k, at] if j == k else re[j] * re[k] + im[j] * im[k]
                    for t in range(terms):
                        sums[t] = add(sums[t], pairs[t, pair] * both)
                    pair += 1
            for t in range(terms):
                qi[s, t, at] = sums[t]
            return carry

        lax.fori_loop(0, tall // CHUNK, body, 0)

    def sweep(s, variance):
        def body(i, total):
            at = pl.ds(pl.multiple_of(i * CHUNK, CHUNK), CHUNK)
            new = refine(est[s, at], [power[s, k, at] for k in range(tapers)], keep, variance)
            est[s, at] = new
            return total + new * weigh[at]

        return lax.fori_loop(0, tall // CHUNK, body, jnp.zeros((CHUNK, LANES), f32))

    def assemble(src):
        mirrored = flip(src[0:rows])

        @pl.when(jnp.logical_not(single))
        def _():
            folded[0] = src[0:rows]
            folded[1] = mirrored

        @pl.when(single)
        def _():
            folded[g, 0 : rows // 2] = src[0 : rows // 2]
            folded[g, rows // 2 : rows // 2 + 1] = src[rows : rows + 1]
            folded[g, rows // 2 + 1 : rows] = mirrored[rows // 2 : rows - 1]
            folded[1 - g, 0 : rows // 2] = mirrored[: rows // 2]
            folded[1 - g, rows // 2 : rows] = src[rows // 2 : rows]

        return folded[0].T, folded[1].T

    def qi_copy(s, t):
        return remote(qi_out.at[s, t], qi_ref.at[g * mine + s, t], qo_ss.at[s], qo_rs.at[s], partner)

    def spec_copy(s):
        return remote(spec_out.at[s], spec_ref.at[g * mine + s], so_ss.at[0], so_rs.at[0], partner)

    def outputs_qi(s):
        for t in range(terms):
            own, sent = assemble(qi.at[s, t])
            qi_out[s, t] = sent
            qi_copy(s, t).start()
            qi_own[s, t] = own
            pltpu.make_async_copy(qi_own.at[s, t], qi_ref.at[g * mine + s, t], own_sem.at[0]).start()

    totals = []
    for s in range(mine):
        for b in batches:
            settle(z_like[s][b], z_rs.at[s, b])
            transform(s, b)
        if s == 0:
            variance0 = first_variance()
        totals.append(measure(s, variance0[s]))
        if s == mine - 1:
            share(0, totals)
        combine(s)
        outputs_qi(s)
    for it in range(1, ITERS):
        if it > 1:
            share(it - 1, totals)
        variance = collect(it - 1)
        totals = [sweep(s, variance[s]) for s in range(mine)]
    for s in range(mine):
        own, sent = assemble(est.at[s])
        spec_out[s] = sent
        spec_copy(s).start()
        spec_own[s] = own
        pltpu.make_async_copy(spec_own.at[s], spec_ref.at[g * mine + s], own_sem.at[1]).start()

    for s in range(mine):
        for b in batches:
            settle(z_like[s][b], z_ss.at[s, b])
    for it in range(ITERS - 1):
        settle(sum_like[it], sum_ss.at[it])
    for s in range(mine):
        settle(qi_out.at[s], qo_rs.at[s])
        settle(qi_out.at[s], qo_ss.at[s])
    settle(qi_own, own_sem.at[0])
    settle(spec_own, own_sem.at[1])
    settle(spec_out, so_rs.at[0])
    settle(spec_out, so_ss.at[0])


def hand_kernel(spec_ref, qi_ref, spec_out, qi_out, spec_held, qi_held, in_sem, out_sem):
    sets = ((spec_ref, spec_held, spec_out), (qi_ref, qi_held, qi_out))
    moves = []
    for i, (src, held, dst) in enumerate(sets):
        for s in range(src.shape[0]):
            enter = pltpu.make_async_copy(src.at[s], held.at[s], in_sem.at[i, s])
            leave = pltpu.make_async_copy(held.at[s], dst.at[s], out_sem.at[i, s])
            enter.start()
            moves.append((enter, leave))
    for enter, leave in moves:
        enter.wait()
        leave.start()
    for _, leave in moves:
        leave.wait()


def local(cores, series, tapers, concentration, qi_weights):
    n = lax.axis_size("af")
    count, local_len = series.shape
    taper_count = tapers.shape[0]
    terms = qi_weights.shape[0]
    half, mine = n // 2, count // 2
    sub_rows = local_len // (half * LANES)
    rows = local_len // LANES
    tall = rows + CHUNK
    sizes = (1,) * (taper_count // cores)
    f32 = jnp.float32
    bf16 = jnp.bfloat16
    smem = pl.BlockSpec(memory_space=pltpu.SMEM)
    hbm = pl.BlockSpec(memory_space=pltpu.HBM)
    dma = pltpu.SemaphoreType.DMA
    shapes = (
        jax.ShapeDtypeStruct((count, LANES, rows), f32),
        jax.ShapeDtypeStruct((count, terms, LANES, rows), f32),
    )
    outs = pl.pallas_call(
        functools.partial(fused_kernel, n, cores, sizes),
        out_shape=shapes,
        in_specs=[hbm, hbm, smem, smem],
        out_specs=(hbm, hbm),
        scratch_shapes=[
            pltpu.VMEM(series.shape, f32),
            pltpu.VMEM(tapers.shape, f32),
            pltpu.VMEM((2, 8 * rows, LANES), f32),
            pltpu.VMEM((count, half, sub_rows, LANES), f32),
            pltpu.VMEM((taper_count, half, sub_rows, LANES), f32),
            pltpu.VMEM((mine, n, sub_rows, LANES), f32),
            pltpu.VMEM((n, taper_count, sub_rows, LANES), f32),
            pltpu.VMEM((half, mine, taper_count, 2, sub_rows, LANES), f32),
            pltpu.VMEM((mine, taper_count, 2, half, sub_rows, LANES), f32),
            pltpu.VMEM((8, LANES), f32),
            pltpu.VMEM((half, 8, LANES), f32),
            pltpu.VMEM((ITERS - 1, 8, LANES), f32),
            pltpu.VMEM((ITERS - 1, half, 8, LANES), f32),
            pltpu.VMEM((2, rows + tall, 2 * rows), bf16),
            pltpu.VMEM((2, 2 * LANES, 2 * LANES), bf16),
            pltpu.VMEM((2, tall, LANES), f32),
            pltpu.VMEM((tall, LANES), f32),
            pltpu.VMEM((2, taper_count, tall, LANES), f32),
            pltpu.VMEM((mine, taper_count, tall, LANES), f32),
            pltpu.VMEM((mine, tall, LANES), f32),
            pltpu.VMEM((mine, terms, tall, LANES), f32),
            pltpu.VMEM((mine, LANES, rows), f32),
            pltpu.VMEM((mine, terms, LANES, rows), f32),
            pltpu.VMEM((mine, LANES, rows), f32),
            pltpu.VMEM((mine, terms, LANES, rows), f32),
            pltpu.SMEM((terms, taper_count * (taper_count + 1) // 2), f32),
            pltpu.VMEM((2, rows, LANES), f32),
            dma((mine,)), dma((mine,)),
            dma((len(sizes),)), dma((len(sizes),)),
            dma((len(sizes),)), dma((len(sizes),)),
            dma((1,)), dma((1,)),
            dma((mine, len(sizes))), dma((mine, len(sizes))),
            dma((ITERS - 1,)), dma((ITERS - 1,)),
            dma((mine,)), dma((mine,)),
            dma((1,)), dma((1,)),
            dma((2,)), dma((2,)),
        ],
        compiler_params=pltpu.CompilerParams(collective_id=0, has_side_effects=True),
    )(series, tapers, concentration, qi_weights.transpose(1, 0, 2))
    spectrum, qi_terms = pl.pallas_call(
        hand_kernel,
        out_shape=shapes,
        in_specs=[hbm, hbm],
        out_specs=(hbm, hbm),
        scratch_shapes=[pltpu.VMEM(shape.shape, f32) for shape in shapes] + [dma((2, count)), dma((2, count))],
    )(*outs)
    return (
        spectrum.reshape(count, 1, local_len),
        qi_terms.reshape(count, terms, 1, local_len),
    )


def solution(mesh):
    placed = (P("sa", "af"), P(None, "af"), P(), P())
    return jax.shard_map(
        functools.partial(local, mesh.shape["sa"]),
        mesh=mesh,
        in_specs=placed,
        out_specs=(P("sa", "af", None), P("sa", None, "af", None)),
        check_vma=False,
    )
```

```python
import functools
import math

import jax
import jax.numpy as jnp
import numpy as np
from jax import lax
from jax.experimental import pallas as pl
from jax.experimental.pallas import tpu as pltpu
from jax.sharding import PartitionSpec as P

ITERS = 3
LANES = 128
CHUNK = 16
MESH = pl.DeviceIdType.MESH


def add(a, b):
    if a is None:
        return b
    return a if b is None else a + b


def sub(a, b):
    if b is None:
        return a
    return -b if a is None else a - b


def butterfly(values):
    n = len(values)
    if n == 1:
        return values
    even, odd = butterfly(values[0::2]), butterfly(values[1::2])
    low, high = [], []
    for k in range(n // 2):
        (er, ei), (tr, ti) = even[k], odd[k]
        if 4 * k == n:
            tr, ti = ti, (None if tr is None else -tr)
        elif k:
            c, s = math.cos(2 * math.pi * k / n), math.sin(2 * math.pi * k / n)
            if ti is None:
                tr, ti = tr * c, tr * (-s)
            else:
                tr, ti = tr * c + ti * s, ti * c - tr * s
        low.append((add(er, tr), add(ei, ti)))
        high.append((sub(er, tr), sub(ei, ti)))
    return low + high


def split(x):
    high = x.astype(jnp.bfloat16)
    return high, (x - high.astype(jnp.float32)).astype(jnp.bfloat16)


def dot3(a, b):
    dot = functools.partial(jnp.dot, preferred_element_type=jnp.float32)
    return dot(a[0], b[0]) + (dot(a[0], b[1]) + dot(a[1], b[0]))


def refine(estimate, powers, keep, variance):
    top = bottom = None
    for k, power in enumerate(powers):
        base = keep[k] * estimate + (1.0 - keep[k]) * variance
        weight = keep[k] / (base * base)
        top = add(top, weight * power)
        bottom = add(bottom, weight)
    return top / bottom


def turn(index, period):
    if period & (period - 1):
        index = lax.rem(index, jnp.full_like(index, period))
    else:
        index = index & (period - 1)
    angle = index.astype(jnp.float32) * (2.0 * math.pi / period)
    return jnp.cos(angle), jnp.sin(angle)


def flip(x):
    rows, lanes = x.shape
    lane = lanes - 1 - lax.broadcasted_iota(jnp.int32, (8, lanes), 1)
    line = 7 - lax.broadcasted_iota(jnp.int32, (8, lanes), 0)
    parts = []
    for i in reversed(range(rows // 8)):
        part = jnp.take_along_axis(x[8 * i : 8 * i + 8], lane, axis=1)
        parts.append(jnp.take_along_axis(part, line, axis=0))
    return jnp.concatenate(parts, axis=0)


def remote(src, dst, send, recv, where):
    return pltpu.make_async_remote_copy(
        src_ref=src, dst_ref=dst, send_sem=send, recv_sem=recv, device_id=where, device_id_type=MESH
    )


def fused_kernel(
    n, cores, sizes, series_hbm, tapers_hbm, keep_ref, mix_ref, spec_ref, qi_ref,
    series_ref, tapers_ref, stage, ser_src, tap_src, ser, tap, zbuf, recv, en_out, en_in, sum_out, sum_in, left, right, inner, weigh,
    spec, power, est, qi, spec_out, qi_out, spec_own, qi_own, pairs, folded,
    ser_ss, ser_rs, tap_ss, tap_rs, core_ss, core_rs, en_ss, en_rs, z_ss, z_rs,
    sum_ss, sum_rs, qo_ss, qo_rs, so_ss, so_rs, in_sem, own_sem,
):
    inputs = [
        pltpu.make_async_copy(series_hbm, series_ref, in_sem.at[0]),
        pltpu.make_async_copy(tapers_hbm, tapers_ref, in_sem.at[1]),
    ]
    for copy in inputs:
        copy.start()
    half = n // 2
    count, sub_rows = ser_src.shape[0], ser_src.shape[2]
    mine = count // 2
    tapers, terms = tap.shape[1], mix_ref.shape[1]
    group = tapers // cores
    batches = range(len(sizes))
    starts = [sum(sizes[:b]) for b in batches]
    places = [cores * start for start in starts]
    order = [c * group + starts[b] + i for b in batches for c in range(cores) for i in range(sizes[b])]
    early = [order.index(0), order.index(1)]
    rows = half * sub_rows
    tall = spec.shape[2]
    extra = tall - rows
    local_len = rows * LANES
    length_all = local_len * n
    tile = min(8, sub_rows)
    f32 = jnp.float32
    me, core = lax.axis_index("af"), lax.axis_index("sa")
    g, h = me // half, lax.rem(me, half)
    peers = [(dg, dh) for dg in (0, 1) for dh in range(half) if dg or dh]
    single = h == 0

    def ahead(dg, dh):
        return lax.rem(g + dg, 2), lax.rem(h + dh, half)

    def flat(at):
        return at[0] * half + at[1]

    def friend(dh):
        return {"af": g * half + lax.rem(h + dh, half)}

    partner = {"af": (1 - g) * half + lax.rem(half - h, half)}
    other_core = lax.rem(core + 1, cores)

    barrier = pltpu.get_barrier_semaphore()
    for dg, dh in peers:
        pl.semaphore_signal(barrier, inc=1, device_id={"af": flat(ahead(dg, dh))}, device_id_type=MESH)
    pl.semaphore_signal(barrier, inc=1, device_id={"sa": other_core}, device_id_type=MESH)

    for copy in inputs:
        copy.wait()
    for j in range(rows):
        lanes = slice(j * LANES, (j + 1) * LANES)
        stage[0, 8 * j : 8 * j + 8] = tapers_ref[0:8, lanes]
        stage[1, 8 * j : 8 * j + tapers - 8] = tapers_ref[8:tapers, lanes]
        stage[1, 8 * j + tapers - 8 : 8 * j + tapers - 8 + count] = series_ref[:, lanes]
    for row in range(tapers + count):
        for j in range(rows // tile):
            part = stage[row // 8, pl.ds(8 * j * tile + row % 8, tile, stride=8)]
            at = (j * tile // sub_rows, slice(j * tile % sub_rows, j * tile % sub_rows + tile))
            if row < tapers:
                tap_src[row, at[0], at[1]] = part
            else:
                ser_src[row - tapers, at[0], at[1]] = part
    pl.semaphore_wait(barrier, n)

    def ser_copy(s, dg, dh):
        to = ahead(dg, dh)
        return remote(
            ser_src.at[to[0] * mine + s, to[1]], ser.at[s, me], ser_ss.at[s], ser_rs.at[s], {"af": flat(to)}
        )

    def tap_copy(b, dg, dh):
        to = ahead(dg, dh)
        return remote(
            tap_src.at[pl.ds(core * group + starts[b], sizes[b]), to[1]],
            tap.at[me, pl.ds(places[b] + core * sizes[b], sizes[b])],
            tap_ss.at[b], tap_rs.at[b], {"af": flat(to)},
        )

    def core_copy(b):
        at = tap.at[:, pl.ds(places[b] + core * sizes[b], sizes[b])]
        return remote(at, at, core_ss.at[b], core_rs.at[b], {"sa": other_core})

    def settle(like, semaphore):
        pltpu.make_async_copy(like, like, semaphore).wait()

    ser_like = [ser.at[s, pl.ds(0, n - 1)] for s in range(mine)]
    carried = [[s for s in range(mine) if (0 if s == 0 else len(sizes) - 1) == b] for b in batches]
    tap_like = [tap.at[pl.ds(0, n - 1), pl.ds(places[b], sizes[b])] for b in batches]
    z_like = [
        [recv.at[s, pl.ds(places[b], cores * sizes[b]), :, pl.ds(0, half - 1)] for b in batches]
        for s in range(mine)
    ]
    en_like = en_in.at[pl.ds(1, half - 1)]
    sum_like = [sum_in.at[it, pl.ds(1, half - 1)] for it in range(ITERS - 1)]

    for b in batches:
        for dg, dh in peers:
            for s in carried[b]:
                ser_copy(s, dg, dh).start()
            tap_copy(b, dg, dh).start()

    for s in range(mine):
        ser[s, me] = ser_src[g * mine + s, h]
    for b in batches:
        for i in range(sizes[b]):
            tap[me, places[b] + core * sizes[b] + i] = tap_src[core * group + starts[b] + i, h]
    for t in range(terms):
        p = 0
        for j in range(tapers):
            for k in range(j, tapers):
                value = mix_ref[order[j], t, order[k]]
                pairs[t, p] = value if j == k else value + mix_ref[order[k], t, order[j]]
                p += 1

    def frequency(shape):
        at = lax.broadcasted_iota(jnp.int32, shape, 0)
        upper = (at >= rows // 2) & (at < rows)
        class_of = jnp.where(single, jnp.where(upper, half, 0), me)
        line = jnp.where(at < rows, at, rows // 2)
        class_of = jnp.where(at < rows, class_of, 0)
        return n * line + class_of, at, upper

    freq, at, upper = frequency((tall, rows))
    c, s = turn(lax.broadcasted_iota(jnp.int32, (tall, rows), 1) * freq, rows * n)
    first = jnp.where(upper, 1, 0) == g
    inside = at < rows
    once = at == rows
    take0 = jnp.where(single, jnp.where(inside | once, jnp.where(first, 1.0, 0.0), 0.0), jnp.where(inside, 1.0, 0.0))
    take1 = jnp.where(single, jnp.where(inside | once, jnp.where(first, 0.0, 1.0), 0.0), 0.0)
    plain = jnp.where(single, 0.0, jnp.where(inside, 1.0, 0.0))
    real0, real1 = c * take0, c * take1 + s * plain
    imag0, imag1 = -(s * take0), c * plain - s * take1
    full = jnp.concatenate(
        [
            jnp.concatenate([real0[:rows], real1[:rows]], axis=1),
            jnp.concatenate([imag0[:rows], imag1[:rows]], axis=1),
            jnp.concatenate([real0[rows:], real1[rows:]], axis=1),
        ],
        axis=0,
    )
    left[0], left[1] = split(full)

    freq, at, upper = frequency((tall, LANES))
    c, s = turn(lax.broadcasted_iota(jnp.int32, (tall, LANES), 1) * freq, length_all)
    scale = 1.0 / math.sqrt(length_all)
    inner[0], inner[1] = c * scale, s * scale
    weigh[...] = jnp.where(
        single,
        jnp.where(at < rows, jnp.where(at == 0, 1.0, 2.0), jnp.where(at == rows, 1.0, 0.0)),
        jnp.where(at < rows, 2.0, 0.0),
    )
    grid = (LANES, LANES)
    c, s = turn(lax.broadcasted_iota(jnp.int32, grid, 0) * lax.broadcasted_iota(jnp.int32, grid, 1), LANES)
    right[0], right[1] = split(
        jnp.concatenate([jnp.concatenate([c, -s], axis=1), jnp.concatenate([s, c], axis=1)], axis=0)
    )
    en_out[...] = jnp.zeros_like(en_out)
    sum_out[...] = jnp.zeros_like(sum_out)

    def arrive(b):
        settle(tap_like[b], tap_rs.at[b])
        core_copy(b).start()
        for s in carried[b]:
            settle(ser_like[s], ser_rs.at[s])
        core_copy(b).wait_recv()

    sign = (1 - 2 * g).astype(f32)

    def front(s, b):
        lo, hi = places[b], places[b] + cores * sizes[b]
        for i in range(sub_rows // tile):
            part = pl.ds(i * tile, tile)

            def body(k, carry):
                got = []
                for p in range(n):
                    value = ser[s, p, part] * tap[p, k, part]
                    got.append((value * sign if p % 2 else value, None))
                out = butterfly(got)
                for u in range(half):
                    re, im = out[u]
                    zbuf[u, s, k, 0, part] = re
                    zbuf[u, s, k, 1, part] = out[half][0] if u == 0 else im
                return carry

            lax.fori_loop(lo, hi, body, 0)
        for k in range(lo, hi):
            for part in range(2):
                recv[s, k, part, h] = zbuf[h, s, k, part]

    def z_copy(s, b, dh):
        to = lax.rem(h + dh, half)
        at = pl.ds(places[b], cores * sizes[b])
        return remote(
            zbuf.at[to, s, at], recv.at[s, at, :, h], z_ss.at[s, b], z_rs.at[s, b], friend(dh)
        )

    def z_start(s, b):
        for dh in range(1, half):
            z_copy(s, b, dh).start()

    def en_copy(dh):
        return remote(en_out, en_in.at[dh], en_ss.at[0], en_rs.at[0], friend(dh))

    def energy(p, total):
        one, two = tap[p, early[0]], tap[p, early[1]]
        new = []
        for s in range(mine):
            a, b = ser[s, p] * one, ser[s, p] * two
            new.append(total[s] + (a * a + b * b))
        return tuple(new)

    for b in batches:
        arrive(b)
        front(0, b)
        if b == len(sizes) - 1:
            total = lax.fori_loop(0, n, energy, tuple(jnp.zeros((sub_rows, LANES), f32) for _ in range(mine)))
            for s in range(mine):
                en_out[s : s + 1] = jnp.sum(total[s], axis=0, keepdims=True)
            for dh in range(1, half):
                en_copy(dh).start()
        z_start(0, b)
    for s in range(1, mine):
        for b in batches:
            front(s, b)
            z_start(s, b)

    for s in range(mine):
        settle(ser_like[s], ser_ss.at[s])
    for b in batches:
        settle(tap_like[b], tap_ss.at[b])
        core_copy(b).wait_send()

    def first_variance():
        settle(en_like, en_rs.at[0])
        settle(en_like, en_ss.at[0])
        total = en_out[...]
        for dh in range(1, half):
            total += en_in[dh]
        return [jnp.sum(total[s : s + 1]) * (0.5 / length_all) for s in range(mine)]

    keep = [keep_ref[k] for k in order]

    def sum_copy(it, dh):
        return remote(sum_out.at[it], sum_in.at[it, dh], sum_ss.at[it], sum_rs.at[it], friend(dh))

    def share(it, totals):
        for s, total in enumerate(totals):
            sum_out[it, s : s + 1] = jnp.sum(total, axis=0, keepdims=True)
        for dh in range(1, half):
            sum_copy(it, dh).start()

    def collect(it):
        settle(sum_like[it], sum_rs.at[it])
        total = sum_out[it]
        for dh in range(1, half):
            total += sum_in[it, dh]
        return [jnp.sum(total[s : s + 1]) / length_all for s in range(mine)]

    def transform(s, b):
        def body(kk, carry):
            k = 2 * kk
            x = jnp.concatenate(
                [recv[s, k].reshape(2 * rows, LANES), recv[s, k + 1].reshape(2 * rows, LANES)], axis=1
            )
            mid = dot3((left[0], left[1]), split(x))
            c, d = inner[0], inner[1]
            turned = []
            for i in range(2):
                lanes = slice(i * LANES, (i + 1) * LANES)
                mr = jnp.concatenate([mid[:rows, lanes], mid[2 * rows :, lanes]], axis=0)
                mi = jnp.concatenate([mid[rows : 2 * rows, lanes], jnp.zeros((extra, LANES), f32)], axis=0)
                turned.append(jnp.concatenate([mr * c + mi * d, mi * c - mr * d], axis=1))
            done = dot3(split(jnp.concatenate(turned, axis=0)), (right[0], right[1]))
            for i in range(2):
                block = done[i * tall : (i + 1) * tall]
                spec[0, k + i] = block[:, :LANES]
                spec[1, k + i] = block[:, LANES:]
            return carry

        lax.fori_loop(places[b] // 2, (places[b] + cores * sizes[b]) // 2, body, 0)

    def measure(s, variance):
        def body(i, total):
            at = pl.ds(pl.multiple_of(i * CHUNK, CHUNK), CHUNK)
            powers = []
            for k in range(tapers):
                re, im = spec[0, k, at], spec[1, k, at]
                powers.append(re * re + im * im)
                power[s, k, at] = powers[k]
            new = refine(0.5 * (powers[early[0]] + powers[early[1]]), powers, keep, variance)
            est[s, at] = new
            return total + new * weigh[at]

        return lax.fori_loop(0, tall // CHUNK, body, jnp.zeros((CHUNK, LANES), f32))

    def combine(s):
        def body(i, carry):
            at = pl.ds(pl.multiple_of(i * CHUNK, CHUNK), CHUNK)
            re = [spec[0, k, at] for k in range(tapers)]
            im = [spec[1, k, at] for k in range(tapers)]
            sums = [None] * terms
            pair = 0
            for j in range(tapers):
                for k in range(j, tapers):
                    both = power[s, k, at] if j == k else re[j] * re[k] + im[j] * im[k]
                    for t in range(terms):
                        sums[t] = add(sums[t], pairs[t, pair] * both)
                    pair += 1
            for t in range(terms):
                qi[s, t, at] = sums[t]
            return carry

        lax.fori_loop(0, tall // CHUNK, body, 0)

    def sweep(s, variance):
        def body(i, total):
            at = pl.ds(pl.multiple_of(i * CHUNK, CHUNK), CHUNK)
            new = refine(est[s, at], [power[s, k, at] for k in range(tapers)], keep, variance)
            est[s, at] = new
            return total + new * weigh[at]

        return lax.fori_loop(0, tall // CHUNK, body, jnp.zeros((CHUNK, LANES), f32))

    def assemble(src):
        mirrored = flip(src[0:rows])

        @pl.when(jnp.logical_not(single))
        def _():
            folded[0] = src[0:rows]
            folded[1] = mirrored

        @pl.when(single)
        def _():
            folded[g, 0 : rows // 2] = src[0 : rows // 2]
            folded[g, rows // 2 : rows // 2 + 1] = src[rows : rows + 1]
            folded[g, rows // 2 + 1 : rows] = mirrored[rows // 2 : rows - 1]
            folded[1 - g, 0 : rows // 2] = mirrored[: rows // 2]
            folded[1 - g, rows // 2 : rows] = src[rows // 2 : rows]

        return folded[0].T, folded[1].T

    def qi_copy(s, t):
        return remote(qi_out.at[s, t], qi_ref.at[g * mine + s, t], qo_ss.at[s], qo_rs.at[s], partner)

    def spec_copy(s):
        return remote(spec_out.at[s], spec_ref.at[g * mine + s], so_ss.at[0], so_rs.at[0], partner)

    def outputs_qi(s, which):
        for t in which:
            own, sent = assemble(qi.at[s, t])
            qi_out[s, t] = sent
            qi_copy(s, t).start()
            qi_own[s, t] = own
            pltpu.make_async_copy(qi_own.at[s, t], qi_ref.at[g * mine + s, t], own_sem.at[0]).start()

    totals = []
    for s in range(mine):
        for b in batches:
            settle(z_like[s][b], z_rs.at[s, b])
            transform(s, b)
            if s:
                outputs_qi(s - 1, [t for t in range(1, terms) if min(t, len(sizes) - 1) == b])
        if s == 0:
            variance0 = first_variance()
        totals.append(measure(s, variance0[s]))
        if s == mine - 1:
            share(0, totals)
        combine(s)
        outputs_qi(s, range(terms) if s == mine - 1 else [0])
    for it in range(1, ITERS):
        if it > 1:
            share(it - 1, totals)
        variance = collect(it - 1)
        totals = [sweep(s, variance[s]) for s in range(mine)]
    for s in range(mine):
        own, sent = assemble(est.at[s])
        spec_out[s] = sent
        spec_copy(s).start()
        spec_own[s] = own
        pltpu.make_async_copy(spec_own.at[s], spec_ref.at[g * mine + s], own_sem.at[1]).start()

    for s in range(mine):
        for b in batches:
            settle(z_like[s][b], z_ss.at[s, b])
    for it in range(ITERS - 1):
        settle(sum_like[it], sum_ss.at[it])
    for s in range(mine):
        settle(qi_out.at[s], qo_rs.at[s])
        settle(qi_out.at[s], qo_ss.at[s])
    settle(qi_own, own_sem.at[0])
    settle(spec_own, own_sem.at[1])
    settle(spec_out, so_rs.at[0])
    settle(spec_out, so_ss.at[0])


def hand_kernel(spec_ref, qi_ref, spec_out, qi_out, spec_held, qi_held, in_sem, out_sem):
    sets = ((spec_ref, spec_held, spec_out), (qi_ref, qi_held, qi_out))
    moves = []
    for i, (src, held, dst) in enumerate(sets):
        for s in range(src.shape[0]):
            enter = pltpu.make_async_copy(src.at[s], held.at[s], in_sem.at[i, s])
            leave = pltpu.make_async_copy(held.at[s], dst.at[s], out_sem.at[i, s])
            enter.start()
            moves.append((enter, leave))
    for enter, leave in moves:
        enter.wait()
        leave.start()
    for _, leave in moves:
        leave.wait()


def local(cores, series, tapers, concentration, qi_weights):
    n = lax.axis_size("af")
    count, local_len = series.shape
    taper_count = tapers.shape[0]
    terms = qi_weights.shape[0]
    half, mine = n // 2, count // 2
    sub_rows = local_len // (half * LANES)
    rows = local_len // LANES
    tall = rows + CHUNK
    sizes = (1,) * (taper_count // cores)
    f32 = jnp.float32
    bf16 = jnp.bfloat16
    smem = pl.BlockSpec(memory_space=pltpu.SMEM)
    hbm = pl.BlockSpec(memory_space=pltpu.HBM)
    dma = pltpu.SemaphoreType.DMA
    shapes = (
        jax.ShapeDtypeStruct((count, LANES, rows), f32),
        jax.ShapeDtypeStruct((count, terms, LANES, rows), f32),
    )
    outs = pl.pallas_call(
        functools.partial(fused_kernel, n, cores, sizes),
        out_shape=shapes,
        in_specs=[hbm, hbm, smem, smem],
        out_specs=(hbm, hbm),
        scratch_shapes=[
            pltpu.VMEM(series.shape, f32),
            pltpu.VMEM(tapers.shape, f32),
            pltpu.VMEM((2, 8 * rows, LANES), f32),
            pltpu.VMEM((count, half, sub_rows, LANES), f32),
            pltpu.VMEM((taper_count, half, sub_rows, LANES), f32),
            pltpu.VMEM((mine, n, sub_rows, LANES), f32),
            pltpu.VMEM((n, taper_count, sub_rows, LANES), f32),
            pltpu.VMEM((half, mine, taper_count, 2, sub_rows, LANES), f32),
            pltpu.VMEM((mine, taper_count, 2, half, sub_rows, LANES), f32),
            pltpu.VMEM((8, LANES), f32),
            pltpu.VMEM((half, 8, LANES), f32),
            pltpu.VMEM((ITERS - 1, 8, LANES), f32),
            pltpu.VMEM((ITERS - 1, half, 8, LANES), f32),
            pltpu.VMEM((2, rows + tall, 2 * rows), bf16),
            pltpu.VMEM((2, 2 * LANES, 2 * LANES), bf16),
            pltpu.VMEM((2, tall, LANES), f32),
            pltpu.VMEM((tall, LANES), f32),
            pltpu.VMEM((2, taper_count, tall, LANES), f32),
            pltpu.VMEM((mine, taper_count, tall, LANES), f32),
            pltpu.VMEM((mine, tall, LANES), f32),
            pltpu.VMEM((mine, terms, tall, LANES), f32),
            pltpu.VMEM((mine, LANES, rows), f32),
            pltpu.VMEM((mine, terms, LANES, rows), f32),
            pltpu.VMEM((mine, LANES, rows), f32),
            pltpu.VMEM((mine, terms, LANES, rows), f32),
            pltpu.SMEM((terms, taper_count * (taper_count + 1) // 2), f32),
            pltpu.VMEM((2, rows, LANES), f32),
            dma((mine,)), dma((mine,)),
            dma((len(sizes),)), dma((len(sizes),)),
            dma((len(sizes),)), dma((len(sizes),)),
            dma((1,)), dma((1,)),
            dma((mine, len(sizes))), dma((mine, len(sizes))),
            dma((ITERS - 1,)), dma((ITERS - 1,)),
            dma((mine,)), dma((mine,)),
            dma((1,)), dma((1,)),
            dma((2,)), dma((2,)),
        ],
        compiler_params=pltpu.CompilerParams(collective_id=0, has_side_effects=True),
    )(series, tapers, concentration, qi_weights.transpose(1, 0, 2))
    spectrum, qi_terms = pl.pallas_call(
        hand_kernel,
        out_shape=shapes,
        in_specs=[hbm, hbm],
        out_specs=(hbm, hbm),
        scratch_shapes=[pltpu.VMEM(shape.shape, f32) for shape in shapes] + [dma((2, count)), dma((2, count))],
    )(*outs)
    return (
        spectrum.reshape(count, 1, local_len),
        qi_terms.reshape(count, terms, 1, local_len),
    )


def solution(mesh):
    placed = (P("sa", "af"), P(None, "af"), P(), P())
    return jax.shard_map(
        functools.partial(local, mesh.shape["sa"]),
        mesh=mesh,
        in_specs=placed,
        out_specs=(P("sa", "af", None), P("sa", None, "af", None)),
        check_vma=False,
    )
```
